128 devices in a mesh: pts: 128 (over y, x, z, core).
Axes of the slice: x: 4, y: 4, z: 4, core: 2. Of those that a mesh axis runs over, the one named last changes fastest.
Arguments:
- point_data: float32 [5, 131072], P(None, 'pts'), may hold values from -1 to 1
- point_counts: int32 [128], P('pts'), may hold values from 64 to 1024, as said below
- point_offsets: int32 [128], P('pts'), may hold values from 0 to 960, as said below
- in_weight: float32 [3, 256], replicated, may hold values from -6 to 6
- input_bias: float32 [256], replicated, may hold values from -3 to 3
- hidden_layer_weight: float32 [3, 256, 256], replicated, may hold values from -0.5 to 0.5
- hidden_bias: float32 [3, 256], replicated, may hold values from -3 to 3
- output_weight: float32 [3, 256], replicated, may hold values from -0.75 to 0.75
- out_bias: float32 [3], replicated, may hold values from -3 to 3
Outputs:
- grad_in_weight: float32 [3, 256], replicated
- grad_in_bias: float32 [256], replicated
- grad_hidden_weight: float32 [3, 256, 256], replicated
- grad_hidden_bias: float32 [3, 256], replicated
- grad_out_weight: float32 [3, 256], replicated
- grad_out_bias: float32 [3], replicated
- term_means: float32 [3], replicated
The draws below stay inside these ranges and needn't reach their ends.
Inputs may be any that keep to these rules, and one draw needn't show every extreme that they name: `point_counts`: some device has exactly 1024 live points and another exactly 64. A device's live points fill its slots point_offsets to point_offsets + point_counts - 1, all within its 1024 slots.
All inputs are finite; a program needn't handle non-finite values.
Results may differ from the reference program's by a relative error of at most 0.0001.
Values sent between devices are 32-bit elements; how exact they have to be, the bound alone decides.
No kernel may reach another device: no remote copies, remote signals or barrier semaphores. Data moves between devices by JAX's collectives and lax.ppermute only.
A program may use at most 64 MiB of HBM per device.

```python
import jax
import jax.numpy as jnp
from jax import lax

WIDTH = 256
HID = 3
CAP = 1024
BLOCK = 256
POINTS = 131072


def shared_layout(key):
    devices = POINTS // CAP
    base = jax.random.randint(jax.random.fold_in(key, 11), (devices,), CAP // 16, CAP + 1)
    fullest = jax.random.randint(jax.random.fold_in(key, 12), (), 0, devices)
    sparsest = (fullest + 1 + jax.random.randint(jax.random.fold_in(key, 14), (), 0, devices - 1)) % devices
    index = jnp.arange(devices)
    counts = jnp.where(index == fullest, CAP, jnp.where(index == sparsest, CAP // 16, base)).astype(jnp.int32)
    offsets = jax.random.randint(jax.random.fold_in(key, 13), (devices,), 0, CAP - counts + 1)
    offsets = jnp.where(index == sparsest, CAP - CAP // 16, offsets).astype(jnp.int32)
    return (counts, offsets)


def draw_point_counts(key, part):
    return shared_layout(key)[0]


def draw_point_offsets(key, part):
    return shared_layout(key)[1]


def levels(rng, dims, split, smallest, top_value):
    gain = 1.0
    for axis_at, blocks in split:
        steps = jax.random.uniform(jax.random.fold_in(jax.random.fold_in(rng, 6), axis_at), (blocks,), jnp.float32, smallest / len(split), top_value / len(split))
        gain = gain * jnp.repeat(jnp.exp(steps), dims[axis_at] // blocks).reshape((-1,) + (1,) * (len(dims) - 1 - axis_at))
    return gain


def normal_values(rng, extent, width, reach, kind=jnp.bfloat16):
    return jnp.clip(width * jax.random.normal(rng, extent, jnp.float32), -reach, reach).astype(kind)


def setup_inputs(seed: int = 0) -> dict:
    splits = jax.random.split(jax.random.key(seed), 10)
    return {
        "point_data": jnp.clip(jax.random.uniform(splits[0], (5, POINTS), jnp.float32, -1.0, 1.0) * levels(splits[0], (5, POINTS), ((1, 128),), -0.4, 0.0), -1.0, 1.0),
        "point_counts": draw_point_counts(jax.random.fold_in(splits[9], 71), 0),
        "point_offsets": draw_point_offsets(jax.random.fold_in(splits[9], 71), 0),
        "in_weight": normal_values(splits[3], (3, WIDTH), 1 ** -0.5, 6.0, jnp.float32),
        "input_bias": normal_values(splits[4], (WIDTH,), 0.5, 3.0, jnp.float32),
        "hidden_layer_weight": normal_values(splits[5], (HID, WIDTH, WIDTH), (WIDTH // 2) ** -0.5, 0.5, jnp.float32),
        "hidden_bias": normal_values(splits[6], (HID, WIDTH), 0.3, 3.0, jnp.float32),
        "output_weight": normal_values(splits[7], (3, WIDTH), (WIDTH // 4) ** -0.5, 0.75, jnp.float32),
        "out_bias": normal_values(splits[8], (3,), 0.5, 3.0, jnp.float32),
    }


viscosity = 0.2
term_weights = (2.0, 1.0, 1.0)
highest_precision = lax.Precision.HIGHEST

def apply_tanh(stack_arrays):
    hidden = jnp.tanh(stack_arrays[0])
    slope = 1.0 - hidden * hidden
    firsts = slope[None] * stack_arrays[1:4]
    seconds = slope[None] * stack_arrays[4:6] - 2.0 * (hidden * slope)[None] * stack_arrays[1:3] * stack_arrays[1:3]
    return jnp.concatenate([hidden[None], firsts, seconds], 0)

def add_bias(stack_arrays, bias):
    return jnp.concatenate([stack_arrays[0:1] + bias[None, :, None], stack_arrays[1:]], 0)

def network_jets(params, coords):
    in_weight, input_bias, hidden_layer_weight, hidden_bias, output_weight, out_bias = params
    rows = coords.shape[1]
    value = jnp.dot(in_weight.T, coords, precision=highest_precision, preferred_element_type=jnp.float32) + input_bias[:, None]
    firsts = in_weight[:, :, None] * jnp.ones((1, 1, rows), jnp.float32)
    zeros = jnp.zeros((2,) + value.shape, jnp.float32)
    stack_arrays = jnp.concatenate([value[None], firsts, zeros], 0)
    for layer_apply in range(hidden_layer_weight.shape[0]):
        stack_arrays = jnp.einsum('hm,xmj->xhj', hidden_layer_weight[layer_apply], apply_tanh(stack_arrays), precision=highest_precision)
        stack_arrays = add_bias(stack_arrays, hidden_bias[layer_apply])
    stack_arrays = jnp.einsum('hm,xmj->xhj', output_weight, apply_tanh(stack_arrays), precision=highest_precision)
    return add_bias(stack_arrays, out_bias)

def residual_totals(params, block_data, mask):
    out = network_jets(params, block_data[0:3])
    x_vel, y_vel = (out[0, 0], out[0, 1])
    continuity = out[1, 0] + out[2, 1]
    momentum_x = out[3, 0] + x_vel * out[1, 0] + y_vel * out[2, 0] + out[1, 2] - viscosity * (out[4, 0] + out[5, 0]) - block_data[3]
    momentum_y = out[3, 1] + x_vel * out[1, 1] + y_vel * out[2, 1] + out[2, 2] - viscosity * (out[4, 1] + out[5, 1]) - block_data[4]
    return jnp.stack([jnp.sum(mask * continuity * continuity), jnp.sum(mask * momentum_x * momentum_x), jnp.sum(mask * momentum_y * momentum_y)])

def reference(point_data, point_counts, point_offsets, in_weight, input_bias, hidden_layer_weight, hidden_bias, output_weight, out_bias):
    params = (in_weight, input_bias, hidden_layer_weight, hidden_bias, output_weight, out_bias)
    slots = jnp.arange(POINTS, dtype=jnp.int32)
    local_slot = slots % CAP
    owner = slots // CAP
    first = point_offsets[owner]
    live = ((local_slot >= first) & (local_slot < first + point_counts[owner])).astype(jnp.float32)
    blocks = POINTS // BLOCK
    data_blocks = jnp.transpose(point_data.reshape(5, blocks, BLOCK), (1, 0, 2))
    mask_blocks = live.reshape(blocks, BLOCK)
    weights = jnp.array(term_weights, jnp.float32)

    def step(carry, inputs):
        sums, grads = carry
        block_data, mask = inputs
        block_sums, pullback = jax.vjp(lambda p: residual_totals(p, block_data, mask), params)
        block_grads = pullback(weights)[0]
        return ((sums + block_sums, jax.tree.map(jnp.add, grads, block_grads)), None)
    start = (jnp.zeros((3,), jnp.float32), jax.tree.map(jnp.zeros_like, params))
    (sums, grads), _ = lax.scan(step, start, (data_blocks, mask_blocks))
    total = jnp.sum(point_counts).astype(jnp.float32)
    return (grads[0] / total, grads[1] / total, grads[2] / total, grads[3] / total, grads[4] / total, grads[5] / total, sums / total)
```

```python
import functools

import jax
import jax.numpy as jnp
from jax import lax
from jax.experimental import pallas as pl
from jax.experimental.pallas import tpu as pltpu
from jax.sharding import Mesh
from jax.sharding import PartitionSpec as P

PTS = ("pts_0", "pts_1", "pts_2", "pts_3")
FAR = ("pts_0", "pts_1", "pts_2")
NEAR = "pts_3"

VISCOSITY = 0.2
BLOCK = 256
WIDTH = 256
ROWS = 16
CHUNKS = WIDTH // ROWS
F32 = jnp.float32
BF16 = jnp.bfloat16
JETS = 5
SMALL_ROW = 3 * 512
PACKED_ROWS = 1664


def split(x):
    high = x.astype(BF16)
    return high, (x - high.astype(F32)).astype(BF16)


def matmul(a, b):
    return lax.dot_general(a, b, (((1,), (0,)), ((), ())), preferred_element_type=F32)


def matmul_nt(a, b):
    return lax.dot_general(a, b, (((1,), (1,)), ((), ())), preferred_element_type=F32)


def fold(x):
    return x[:, :128] + x[:, 128:]


def step_kernel(
    counts_ref,
    offsets_ref,
    data_ref,
    in_w_ref,
    in_b_ref,
    hid_w_ref,
    hid_b_ref,
    out_w_ref,
    out_b_ref,
    packed_ref,
    w_cat,
    wt_cat,
    w0_cat,
    wt0_cat,
    out_cat,
    cols,
    z_buf,
    h_buf,
    s_buf,
    q_buf,
    ah_buf,
    al_buf,
    a0h_buf,
    a0l_buf,
    a3_buf,
    g_buf,
    dzh_buf,
    dzl_buf,
    grad_w,
    grad_g,
    partial,
    sums_buf,
):
    live_start = offsets_ref[0]
    live_count = counts_ref[0]
    first_block = live_start // BLOCK
    end_block = (live_start + live_count + BLOCK - 1) // BLOCK

    def put_cat(ref, index, value):
        high, low = split(value)
        ref[index, :, 0:256] = high
        ref[index, :, 256:512] = low
        ref[index, :, 512:768] = high

    wx = in_w_ref[0:1, :]
    wy = in_w_ref[1:2, :]
    wt = in_w_ref[2:3, :]
    wl = wx * wx + wy * wy
    for layer in (1, 2):
        w = hid_w_ref[layer]
        put_cat(w_cat, layer - 1, w)
        put_cat(wt_cat, layer - 1, w.T)
    w0 = hid_w_ref[0]
    for jet, scaled in enumerate((w0, w0 * wx, w0 * wy, w0 * wt, w0 * wl)):
        put_cat(w0_cat, jet, scaled)
        put_cat(wt0_cat, jet, scaled.T)
    out_high, out_low = split(out_w_ref[...])
    out_cat[...] = jnp.zeros_like(out_cat)
    out_cat[0:3, 0:256] = out_high
    out_cat[0:3, 256:512] = out_high
    out_cat[16:19, 0:256] = out_low
    rows = jnp.concatenate(
        [
            in_w_ref[...],
            in_b_ref[...],
            hid_b_ref[...],
            out_w_ref[...],
            jnp.zeros((6, WIDTH), F32),
        ],
        axis=0,
    )
    columns = rows.T
    for i in range(10):
        cols[i] = jnp.broadcast_to(columns[:, i : i + 1], (WIDTH, 128))
    grad_w[...] = jnp.zeros_like(grad_w)
    grad_g[...] = jnp.zeros_like(grad_g)
    partial[...] = jnp.zeros_like(partial)
    sums_buf[...] = jnp.zeros_like(sums_buf)

    def wide(i, r):
        c = cols[i, r, :]
        return jnp.concatenate([c, c], axis=1)

    chunks = [slice(c * ROWS, (c + 1) * ROWS) for c in range(CHUNKS)]

    def block(index, carry):
        base = pl.multiple_of(index * BLOCK, BLOCK)
        points = data_ref[:, pl.ds(base, BLOCK)]
        px = points[0:1, :]
        py = points[1:2, :]
        pt = points[2:3, :]
        slots = base + lax.broadcasted_iota(jnp.int32, (1, BLOCK), 1)
        mask = ((slots >= live_start) & (slots < live_start + live_count)).astype(F32)

        for r in chunks:
            z = wide(0, r) * px + wide(1, r) * py + wide(2, r) * pt + wide(3, r)
            h = jnp.tanh(z)
            s = 1.0 - h * h
            q = -2.0 * h * s
            h_buf[0, r, :] = h
            s_buf[0, r, :] = s
            for i, a in enumerate((h, s, q)):
                high, low = split(a)
                a0h_buf[i, r, :] = high
                a0l_buf[i, r, :] = low

        def forward_dot(layer, jet):
            if layer == 0:
                source = (0, 1, 1, 1, 2)[jet]
                high = a0h_buf[source]
                low = a0l_buf[source]
                w = w0_cat[jet]
            else:
                high = ah_buf[layer - 1, jet]
                low = al_buf[layer - 1, jet]
                w = w_cat[layer - 1]
            return matmul(w, jnp.concatenate([high, high, low], axis=0))

        for layer in range(3):
            top = layer == 2

            def put(jet, r, a):
                high, low = split(a)
                ah_buf[layer, jet, r, :] = high
                al_buf[layer, jet, r, :] = low
                if top:
                    a3_buf[jet, r, :] = a

            for jet in range(JETS):
                z_buf[layer, jet] = forward_dot(layer, jet)
            for r in chunks:
                h = jnp.tanh(z_buf[layer, 0, r, :] + wide(4 + layer, r))
                s = 1.0 - h * h
                q = -2.0 * h * s
                h_buf[layer + 1, r, :] = h
                s_buf[layer + 1, r, :] = s
                q_buf[layer, r, :] = q
                put(0, r, h)
            for jet in (1, 2, 3):
                for r in chunks:
                    put(jet, r, s_buf[layer + 1, r, :] * z_buf[layer, jet, r, :])
            for r in chunks:
                zx = z_buf[layer, 1, r, :]
                zy = z_buf[layer, 2, r, :]
                a = s_buf[layer + 1, r, :] * z_buf[layer, 4, r, :] + q_buf[layer, r, :] * (
                    zx * zx + zy * zy
                )
                put(4, r, a)

        outs = []
        for jet in range(JETS):
            both = matmul(
                out_cat[...],
                jnp.concatenate([ah_buf[2, jet], al_buf[2, jet]], axis=0),
            )
            outs.append(both[0:8] + both[16:24])
        u = outs[0][0:1] + out_b_ref[0]
        v = outs[0][1:2] + out_b_ref[1]
        u_x, v_x, p_x = outs[1][0:1], outs[1][1:2], outs[1][2:3]
        u_y, v_y, p_y = outs[2][0:1], outs[2][1:2], outs[2][2:3]
        u_t, v_t = outs[3][0:1], outs[3][1:2]
        u_l, v_l = outs[4][0:1], outs[4][1:2]
        cont = mask * (u_x + v_y)
        mom_x = mask * (u_t + u * u_x + v * u_y + p_x - VISCOSITY * u_l - points[3:4, :])
        mom_y = mask * (v_t + u * v_x + v * v_y + p_y - VISCOSITY * v_l - points[4:5, :])
        gc = 4.0 * cont
        gx = 2.0 * mom_x
        gy = 2.0 * mom_y
        du = gx * u_x + gy * v_x
        dv = gx * u_y + gy * v_y
        du_x = gc + gx * u
        dv_x = gy * u
        du_y = gx * v
        dv_y = gc + gy * v
        sums_buf[0:1, :] += cont * cont
        sums_buf[1:2, :] += mom_x * mom_x
        sums_buf[2:3, :] += mom_y * mom_y
        sums_buf[3:4, :] += du
        sums_buf[4:5, :] += dv

        def activation_back(a, r, g):
            h = h_buf[a, r, :]
            s = s_buf[a, r, :]
            zx = z_buf[a - 1, 1, r, :]
            zy = z_buf[a - 1, 2, r, :]
            zt = z_buf[a - 1, 3, r, :]
            zl = z_buf[a - 1, 4, r, :]
            g0, g1, g2, g3, g4 = g
            qg = 2.0 * (q_buf[a - 1, r, :] * g4)
            d_s = zx * g1 + zy * g2 + zt * g3 + zl * g4
            d_q = (zx * zx + zy * zy) * g4
            d0 = s * (g0 - 2.0 * (h * d_s) + (4.0 - 6.0 * s) * d_q)
            d1 = s * g1 + qg * zx
            d2 = s * g2 + qg * zy
            d3 = s * g3
            d4 = s * g4
            partial[a - 1, r, :] += fold(d0)
            for jet, d in enumerate((d0, d1, d2, d3, d4)):
                high, low = split(d)
                dzh_buf[a - 1, jet, r, :] = high
                dzl_buf[a - 1, jet, r, :] = low

        for r in chunks:
            wu = wide(7, r)
            wv = wide(8, r)
            wp = wide(9, r)
            g3 = wu * gx + wv * gy
            activation_back(
                3,
                r,
                (
                    wu * du + wv * dv,
                    wu * du_x + wv * dv_x + wp * gx,
                    wu * du_y + wv * dv_y + wp * gy,
                    g3,
                    -VISCOSITY * g3,
                ),
            )
            a0 = a3_buf[0, r, :]
            a1 = a3_buf[1, r, :]
            a2 = a3_buf[2, r, :]
            a34 = a3_buf[3, r, :] - VISCOSITY * a3_buf[4, r, :]
            partial[7, r, :] += fold(a0 * du + a1 * du_x + a2 * du_y + a34 * gx)
            partial[8, r, :] += fold(a0 * dv + a1 * dv_x + a2 * dv_y + a34 * gy)
            partial[9, r, :] += fold(a1 * gx + a2 * gy)

        for layer in (2, 1):
            for jet in range(JETS):
                high = dzh_buf[layer, jet]
                low = dzl_buf[layer, jet]
                g_buf[layer, jet] = matmul(
                    wt_cat[layer - 1], jnp.concatenate([high, high, low], axis=0)
                )
            left, right = [], []
            for jet in range(JETS):
                high = dzh_buf[layer, jet]
                left += [high, dzl_buf[layer, jet], high]
                a_high = ah_buf[layer - 1, jet]
                right += [a_high, a_high, al_buf[layer - 1, jet]]
            grad_w[layer - 1] += matmul_nt(
                jnp.concatenate(left, axis=1), jnp.concatenate(right, axis=1)
            )
            for r in chunks:
                activation_back(layer, r, [g_buf[layer, jet, r, :] for jet in range(JETS)])

        def stacked(jet):
            high = dzh_buf[0, jet]
            return [high, high, dzl_buf[0, jet]]

        g_buf[0, 0] = matmul(wt0_cat[0], jnp.concatenate(stacked(0), axis=0))
        g_buf[0, 1] = matmul(
            jnp.concatenate([wt0_cat[1], wt0_cat[2], wt0_cat[3]], axis=1),
            jnp.concatenate(stacked(1) + stacked(2) + stacked(3), axis=0),
        )
        g_buf[0, 2] = matmul(wt0_cat[4], jnp.concatenate(stacked(4), axis=0))
        for jet in range(JETS):
            source = (0, 1, 1, 1, 2)[jet]
            high = dzh_buf[0, jet]
            a_high = a0h_buf[source]
            grad_g[jet] += matmul_nt(
                jnp.concatenate([high, dzl_buf[0, jet], high], axis=1),
                jnp.concatenate([a_high, a_high, a0l_buf[source]], axis=1),
            )
        for r in chunks:
            h = h_buf[0, r, :]
            s = s_buf[0, r, :]
            d = s * (
                g_buf[0, 0, r, :]
                - 2.0 * (h * g_buf[0, 1, r, :])
                + (4.0 - 6.0 * s) * g_buf[0, 2, r, :]
            )
            partial[3, r, :] += fold(d * px)
            partial[4, r, :] += fold(d * py)
            partial[5, r, :] += fold(d * pt)
            partial[6, r, :] += fold(d)
        return carry

    lax.fori_loop(first_block, end_block, block, 0)

    def put_matrix(slot, value):
        packed_ref[slot * 512 : slot * 512 + 256, :] = value[:, :128]
        packed_ref[slot * 512 + 256 : slot * 512 + 512, :] = value[:, 128:]

    put_matrix(1, grad_w[0])
    put_matrix(2, grad_w[1])
    put_matrix(
        0,
        grad_g[0]
        + grad_g[1] * wx
        + grad_g[2] * wy
        + grad_g[3] * wt
        + grad_g[4] * wl,
    )
    by_l = 2.0 * jnp.sum(w0 * grad_g[4], axis=0, keepdims=True)
    direct = [
        jnp.sum(w0 * grad_g[1], axis=0, keepdims=True) + by_l * wx,
        jnp.sum(w0 * grad_g[2], axis=0, keepdims=True) + by_l * wy,
        jnp.sum(w0 * grad_g[3], axis=0, keepdims=True),
    ]
    lanes = lax.broadcasted_iota(jnp.int32, (WIDTH, 128), 1)
    placed = jnp.zeros((WIDTH, 128), F32)
    for i in range(10):
        placed = jnp.where(lanes == i, jnp.sum(partial[i], axis=1, keepdims=True), placed)
    small = placed.T[0:16]
    small_rows = [small[i : i + 1] for i in range(10)]
    for k in range(3):
        small_rows[3 + k] = small_rows[3 + k] + direct[k]
    totals = jnp.sum(sums_buf[...], axis=1, keepdims=True)
    lane = lax.broadcasted_iota(jnp.int32, (1, WIDTH), 1)
    scalars = jnp.where(lane == 6, live_count.astype(F32), 0.0)
    for at, row in ((0, 0), (1, 1), (2, 2), (3, 3), (4, 4)):
        scalars = jnp.where(lane == at, totals[row : row + 1], scalars)
    small_rows.append(scalars)
    block_small = jnp.concatenate(small_rows + [jnp.zeros((5, WIDTH), F32)], axis=0)
    packed_ref[SMALL_ROW : SMALL_ROW + 16, :] = block_small[:, :128]
    packed_ref[SMALL_ROW + 16 : SMALL_ROW + 32, :] = block_small[:, 128:]
    packed_ref[SMALL_ROW + 32 :, :] = jnp.zeros((PACKED_ROWS - SMALL_ROW - 32, 128), F32)


def local_terms(counts, offsets, data, in_w, in_b, hid_w, hid_b, out_w, out_b):
    vmem = pl.BlockSpec(memory_space=pltpu.VMEM)
    smem = pl.BlockSpec(memory_space=pltpu.SMEM)
    square = (WIDTH, BLOCK)
    return pl.pallas_call(
        step_kernel,
        out_shape=jax.ShapeDtypeStruct((PACKED_ROWS, 128), F32),
        in_specs=[smem, smem, vmem, vmem, vmem, vmem, vmem, vmem, smem],
        out_specs=vmem,
        scratch_shapes=[
            pltpu.VMEM((2, WIDTH, 768), BF16),
            pltpu.VMEM((2, WIDTH, 768), BF16),
            pltpu.VMEM((5, WIDTH, 768), BF16),
            pltpu.VMEM((5, WIDTH, 768), BF16),
            pltpu.VMEM((32, 512), BF16),
            pltpu.VMEM((10, WIDTH, 128), F32),
            pltpu.VMEM((3, JETS) + square, F32),
            pltpu.VMEM((4,) + square, F32),
            pltpu.VMEM((4,) + square, F32),
            pltpu.VMEM((3,) + square, F32),
            pltpu.VMEM((3, JETS) + square, BF16),
            pltpu.VMEM((3, JETS) + square, BF16),
            pltpu.VMEM((3,) + square, BF16),
            pltpu.VMEM((3,) + square, BF16),
            pltpu.VMEM((JETS,) + square, F32),
            pltpu.VMEM((3, JETS) + square, F32),
            pltpu.VMEM((3, JETS) + square, BF16),
            pltpu.VMEM((3, JETS) + square, BF16),
            pltpu.VMEM((2, WIDTH, WIDTH), F32),
            pltpu.VMEM((JETS, WIDTH, WIDTH), F32),
            pltpu.VMEM((10, WIDTH, 128), F32),
            pltpu.VMEM((8, BLOCK), F32),
        ],
        compiler_params=pltpu.CompilerParams(vmem_limit_bytes=60 * 1024 * 1024),
        name="pinn_step",
    )(counts, offsets, data, in_w, in_b.reshape(1, WIDTH), hid_w, hid_b, out_w, out_b)


def unpack_kernel(total_ref, in_w, in_b, hid_w, hid_b, out_w, out_b, means):
    scalars = total_ref[SMALL_ROW + 10 : SMALL_ROW + 11, :]
    scale = 1.0 / scalars[0:1, 6:7]
    for slot in range(3):
        hid_w[slot, :, 0:128] = total_ref[slot * 512 : slot * 512 + 256, :] * scale
        hid_w[slot, :, 128:256] = total_ref[slot * 512 + 256 : slot * 512 + 512, :] * scale

    def rows(first, count):
        at = SMALL_ROW + first
        left = total_ref[at : at + count, :]
        right = total_ref[at + 16 : at + 16 + count, :]
        return jnp.concatenate([left, right], axis=1) * scale

    hid_b[...] = rows(0, 3)
    in_w[...] = rows(3, 3)
    in_b[...] = rows(6, 1)
    out_w[...] = rows(7, 3)
    scaled = scalars * scale
    means[...] = scaled
    out_b[...] = scaled


def unpacked(total):
    vmem = pl.BlockSpec(memory_space=pltpu.VMEM)
    shapes = [(3, WIDTH), (1, WIDTH), (3, WIDTH, WIDTH), (3, WIDTH), (3, WIDTH), (1, 128), (1, 128)]
    in_w, in_b, hid_w, hid_b, out_w, out_b, means = pl.pallas_call(
        unpack_kernel,
        out_shape=[jax.ShapeDtypeStruct(s, F32) for s in shapes],
        in_specs=[vmem],
        out_specs=[vmem] * 7,
        name="unpack",
    )(total)
    return (
        in_w,
        in_b.reshape(WIDTH),
        hid_w,
        hid_b,
        out_w,
        out_b[0, 3:6],
        means[0, 0:3],
    )


def summed_over_devices(packed):
    half = PACKED_ROWS // 2
    core = lax.axis_index(NEAR)
    both = packed.reshape(2, half, 128)
    given = lax.dynamic_index_in_dim(both, 1 - core, 0, False)
    kept = lax.dynamic_index_in_dim(both, core, 0, False)
    mine = kept + lax.ppermute(given, NEAR, [(0, 1), (1, 0)])
    members = lax.axis_size(FAR)
    parts = lax.all_to_all(mine.reshape(members, half // members, 128), FAR, 0, 0, tiled=True)
    own = parts.sum(axis=0)
    spread = jnp.broadcast_to(own[None], (members,) + own.shape)
    gathered = lax.all_to_all(spread, FAR, 0, 0, tiled=True).reshape(half, 128)
    return lax.all_gather(gathered, NEAR, axis=0, tiled=True)


def shards(
    point_data,
    point_counts,
    point_offsets,
    in_weight,
    input_bias,
    hidden_layer_weight,
    hidden_bias,
    output_weight,
    out_bias,
):
    packed = local_terms(
        point_counts,
        point_offsets,
        point_data,
        in_weight,
        input_bias,
        hidden_layer_weight,
        hidden_bias,
        output_weight,
        out_bias,
    )
    return unpacked(summed_over_devices(packed))


def solution(mesh):
    torus = Mesh(mesh.devices.reshape(4, 4, 4, 2), PTS)
    placed = (P(None, PTS), P(PTS), P(PTS), P(), P(), P(), P(), P(), P())
    return jax.shard_map(
        shards,
        mesh=torus,
        in_specs=placed,
        out_specs=(P(), P(), P(), P(), P(), P(), P()),
        check_vma=False,
    )
```

```python
import functools

import jax
import jax.numpy as jnp
from jax import lax
from jax.experimental import pallas as pl
from jax.experimental.pallas import tpu as pltpu
from jax.sharding import Mesh
from jax.sharding import PartitionSpec as P

PTS = ("pts_0", "pts_1", "pts_2", "pts_3")
FAR = ("pts_0", "pts_1", "pts_2")
NEAR = "pts_3"

VISCOSITY = 0.2
HALF = 256
WIDTH = 256
ROWS = 16
F32 = jnp.float32
BF16 = jnp.bfloat16
JETS = 4
SMALL_ROW = 3 * 512
PACKED_ROWS = 1664
HALF_ROWS = PACKED_ROWS // 2
TILES = [
    (slice(r * ROWS, (r + 1) * ROWS), slice(c * 128, (c + 1) * 128))
    for r in range(WIDTH // ROWS)
    for c in range(HALF // 128)
]
PAIRS = 2


def split(x):
    high = x.astype(BF16)
    return high, (x - high.astype(F32)).astype(BF16)


def matmul(a, b):
    return lax.dot_general(a, b, (((1,), (0,)), ((), ())), preferred_element_type=F32)


def matmul_nt(a, b):
    return lax.dot_general(a, b, (((1,), (1,)), ((), ())), preferred_element_type=F32)


def step_kernel(
    core_ref,
    counts_ref,
    offsets_ref,
    data_ref,
    in_w_ref,
    in_b_ref,
    hid_w_ref,
    hid_b_ref,
    out_w_ref,
    out_b_ref,
    kept_ref,
    given_ref,
    w_cat,
    wt_cat,
    out_cat,
    outt_cat,
    cols,
    rows_buf,
    z_buf,
    h_buf,
    ah_buf,
    al_buf,
    a0h_buf,
    a0l_buf,
    g_buf,
    dzh_buf,
    dzl_buf,
    grads,
    partial,
    grad_out,
    sums_buf,
):
    live_start = offsets_ref[0]
    live_count = counts_ref[0]
    first_block = live_start // (2 * HALF * (PAIRS // 2))
    end_block = (live_start + live_count + 2 * HALF - 1) // (2 * HALF)

    def put_cat(ref, index, value):
        high, low = split(value)
        ref[index, :, 0:256] = high
        ref[index, :, 256:512] = low
        ref[index, :, 512:768] = high

    wx = in_w_ref[0:1, :]
    wy = in_w_ref[1:2, :]
    w0 = hid_w_ref[0]
    for index, w in enumerate((w0, w0 * wx, w0 * wy, hid_w_ref[1], hid_w_ref[2])):
        put_cat(w_cat, index, w)
        put_cat(wt_cat, index, w.T)
    out_high, out_low = split(out_w_ref[...])
    out_cat[...] = jnp.zeros_like(out_cat)
    out_cat[0:3, 0:256] = out_high
    out_cat[0:3, 256:512] = out_high
    out_cat[16:19, 0:256] = out_low
    spare = jnp.zeros((5, WIDTH), F32)
    out_rows = jnp.concatenate(
        [out_high.astype(F32), spare, out_low.astype(F32), spare, out_high.astype(F32), spare, jnp.zeros((8, WIDTH), F32)],
        axis=0,
    )
    outt_cat[...] = out_rows.T.astype(BF16)
    rows = jnp.concatenate(
        [
            in_w_ref[...],
            in_b_ref[...],
            hid_b_ref[...],
            wx * wx + wy * wy,
        ],
        axis=0,
    )
    columns = rows.T
    for i in range(8):
        cols[i] = jnp.broadcast_to(columns[:, i : i + 1], (WIDTH, 128))
    grads[...] = jnp.zeros_like(grads)
    partial[...] = jnp.zeros_like(partial)
    sums_buf[...] = jnp.zeros_like(sums_buf)
    grad_out[...] = jnp.zeros_like(grad_out)

    def chain(base, at):
        points = data_ref[:, pl.ds(base, HALF)]
        slots = base + lax.broadcasted_iota(jnp.int32, (1, HALF), 1)
        mask = ((slots >= live_start) & (slots < live_start + live_count)).astype(F32)

        def spread(i, row):
            rows_buf[at, i] = jnp.broadcast_to(row, (8, HALF))

        def row(i, lane):
            tile = rows_buf[at, i, :, lane]
            return jnp.concatenate([tile, tile], axis=0)

        for i in range(3):
            spread(i, points[i : i + 1, :])

        def put_split(high_ref, low_ref, where, value):
            high, low = split(value)
            high_ref[where] = high
            low_ref[where] = low

        for r, l in TILES:
            z = cols[0, r] * row(0, l) + cols[1, r] * row(1, l) + cols[2, r] * row(2, l) + cols[3, r]
            h = jnp.tanh(z)
            s = 1.0 - h * h
            h_buf[at, 0, r, l] = h
            d = s * cols[2, r] + (2.0 * VISCOSITY) * (h * s) * cols[7, r]
            for i, a in enumerate((h, s, d)):
                put_split(a0h_buf, a0l_buf, (at, i, r, l), a)
        yield

        def source(layer, jet):
            if layer == 0:
                i = (0, 1, 1, 2)[jet]
                return a0h_buf[at, i], a0l_buf[at, i]
            return ah_buf[at, layer - 1, jet], al_buf[at, layer - 1, jet]

        for layer in range(3):
            for jet in range(JETS):
                high, low = source(layer, jet)
                w = w_cat[(0, 1, 2, 0)[jet]] if layer == 0 else w_cat[layer + 2]
                z_buf[at, layer, jet] = matmul(w, jnp.concatenate([high, high, low], axis=0))
            yield
            for r, l in TILES:
                h = jnp.tanh(z_buf[at, layer, 0, r, l] + cols[4 + layer, r])
                s = 1.0 - h * h
                h_buf[at, layer + 1, r, l] = h
                zx = z_buf[at, layer, 1, r, l]
                zy = z_buf[at, layer, 2, r, l]
                d = s * z_buf[at, layer, 3, r, l] + (2.0 * VISCOSITY) * (h * s) * (
                    zx * zx + zy * zy
                )
                for jet, a in enumerate((h, s * zx, s * zy, d)):
                    put_split(ah_buf, al_buf, (at, layer, jet, r, l), a)
            yield

        outs = []
        for jet in range(JETS):
            high, low = source(3, jet)
            both = matmul(out_cat[...], jnp.concatenate([high, low], axis=0))
            outs.append(both[0:8] + both[16:24])
        u = outs[0][0:1] + out_b_ref[0]
        v = outs[0][1:2] + out_b_ref[1]
        u_x, v_x, p_x = outs[1][0:1], outs[1][1:2], outs[1][2:3]
        u_y, v_y, p_y = outs[2][0:1], outs[2][1:2], outs[2][2:3]
        u_d, v_d = outs[3][0:1], outs[3][1:2]
        cont = mask * (u_x + v_y)
        mom_x = mask * (u_d + u * u_x + v * u_y + p_x - points[3:4, :])
        mom_y = mask * (v_d + u * v_x + v * v_y + p_y - points[4:5, :])
        gc = 4.0 * cont
        gx = 2.0 * mom_x
        gy = 2.0 * mom_y
        du = gx * u_x + gy * v_x
        dv = gx * u_y + gy * v_y
        nothing = jnp.zeros_like(gx)
        cotangents = [
            jnp.concatenate([a, b, c] + [nothing] * 5, axis=0)
            for a, b, c in (
                (du, dv, nothing),
                (gc + gx * u, gy * u, gx),
                (gx * v, gc + gy * v, gy),
                (gx, gy, nothing),
            )
        ]
        sums_buf[0:1, :] += cont * cont
        sums_buf[1:2, :] += mom_x * mom_x
        sums_buf[2:3, :] += mom_y * mom_y
        sums_buf[3:4, :] += du
        sums_buf[4:5, :] += dv
        left, right = [], []
        for jet, value in enumerate(cotangents):
            high = value.astype(BF16).astype(F32)
            low = value - high
            g_buf[at, jet] = matmul(
                outt_cat[...],
                jnp.concatenate([high, high, low, jnp.zeros_like(low)], axis=0).astype(BF16),
            )
            pad = jnp.zeros_like(high)
            both = jnp.concatenate([high, pad, low, pad], axis=0).astype(BF16)
            alone = jnp.concatenate([high, pad, pad, pad], axis=0).astype(BF16)
            a_high, a_low = source(3, jet)
            left += [both, alone]
            right += [a_high, a_low]
        grad_out[...] += matmul_nt(jnp.concatenate(left, axis=1), jnp.concatenate(right, axis=1))
        yield

        def activation_back(a, r, l):
            h = h_buf[at, a, r, l]
            s = 1.0 - h * h
            zx = z_buf[at, a - 1, 1, r, l]
            zy = z_buf[at, a - 1, 2, r, l]
            zd = z_buf[at, a - 1, 3, r, l]
            square = zx * zx + zy * zy
            q = (2.0 * VISCOSITY) * (h * s)
            g0, g1, g2, g3 = [g_buf[at, jet, r, l] for jet in range(JETS)]
            qg = 2.0 * (q * g3)
            d_s = zx * g1 + zy * g2 + zd * g3
            d_q = square * g3
            d0 = s * (g0 - 2.0 * (h * d_s) + (6.0 * VISCOSITY * s - 4.0 * VISCOSITY) * d_q)
            d1 = s * g1 + qg * zx
            d2 = s * g2 + qg * zy
            partial[a - 1, r] += d0
            for jet, d in enumerate((d0, d1, d2, s * g3)):
                put_split(dzh_buf, dzl_buf, (at, a % 2, jet, r, l), d)

        for r, l in TILES:
            activation_back(3, r, l)
        yield

        for layer in (2, 1):
            up = (layer + 1) % 2
            for jet in range(JETS):
                high = dzh_buf[at, up, jet]
                g_buf[at, jet] = matmul(
                    wt_cat[layer + 2],
                    jnp.concatenate([high, high, dzl_buf[at, up, jet]], axis=0),
                )
            left, right = [], []
            for jet in range(JETS):
                high = dzh_buf[at, up, jet]
                left += [high, dzl_buf[at, up, jet], high]
                a_high, a_low = source(layer, jet)
                right += [a_high, a_high, a_low]
            grads[layer + 2] += matmul_nt(
                jnp.concatenate(left, axis=1), jnp.concatenate(right, axis=1)
            )
            yield
            for r, l in TILES:
                activation_back(layer, r, l)
            yield

        def stacked(jet):
            high = dzh_buf[at, 1, jet]
            return [high, high, dzl_buf[at, 1, jet]]

        g_buf[at, 0] = matmul(wt_cat[0], jnp.concatenate(stacked(0), axis=0))
        g_buf[at, 1] = matmul(
            jnp.concatenate([wt_cat[1], wt_cat[2]], axis=1),
            jnp.concatenate(stacked(1) + stacked(2), axis=0),
        )
        g_buf[at, 2] = matmul(wt_cat[0], jnp.concatenate(stacked(3), axis=0))
        for index, jets in enumerate(((0, 3), (1,), (2,))):
            left, right = [], []
            for jet in jets:
                high = dzh_buf[at, 1, jet]
                left += [high, dzl_buf[at, 1, jet], high]
                a_high, a_low = source(0, jet)
                right += [a_high, a_high, a_low]
            grads[index] += matmul_nt(
                jnp.concatenate(left, axis=1), jnp.concatenate(right, axis=1)
            )
        yield
        for r, l in TILES:
            h = h_buf[at, 0, r, l]
            s = 1.0 - h * h
            g3 = g_buf[at, 2, r, l]
            d_s = g_buf[at, 1, r, l] + cols[2, r] * g3
            d_q = cols[7, r] * g3
            d = s * (
                g_buf[at, 0, r, l]
                - 2.0 * (h * d_s)
                + (6.0 * VISCOSITY * s - 4.0 * VISCOSITY) * d_q
            )
            partial[3, r] += d * row(0, l)
            partial[4, r] += d * row(1, l)
            partial[5, r] += d * row(2, l) + s * g3
            partial[6, r] += d
            partial[7, r] += (2.0 * VISCOSITY) * (h * s) * g3
        yield

    def run(chains):
        queues = [[chains[i] for i in range(k, len(chains), 2)] for k in range(2)]
        started = False
        while any(queues):
            for k, queue in enumerate(queues):
                if k == 1 and not started:
                    started = True
                    continue
                while queue:
                    try:
                        next(queue[0])
                        break
                    except StopIteration:
                        queue.pop(0)

    if PAIRS == 4:
        run([chain(i * HALF, i % 2) for i in range(4)])
    else:

        def block(index, carry):
            base = pl.multiple_of(index * (2 * HALF), 2 * HALF)
            run([chain(pl.multiple_of(base + i * HALF, HALF), i) for i in range(2)])
            return carry

        lax.fori_loop(first_block, end_block, block, 0)

    wt = in_w_ref[2:3, :]
    grad0 = grads[0] + grads[1] * wx + grads[2] * wy
    direct = [
        jnp.sum(w0 * grads[1], axis=0, keepdims=True),
        jnp.sum(w0 * grads[2], axis=0, keepdims=True),
    ]
    lanes = lax.broadcasted_iota(jnp.int32, (WIDTH, 128), 1)
    placed = jnp.zeros((WIDTH, 128), F32)
    for i in range(8):
        placed = jnp.where(lanes == i, jnp.sum(partial[i], axis=1, keepdims=True), placed)
    small = placed.T[0:16]
    small_rows = [small[i : i + 1] for i in range(7)]
    small_rows.append(grad_out[0:3, :] + grad_out[16:19, :])
    by_square = 2.0 * small[7:8]
    small_rows[3] = small_rows[3] + direct[0] + by_square * wx
    small_rows[4] = small_rows[4] + direct[1] + by_square * wy
    totals = jnp.sum(sums_buf[...], axis=1, keepdims=True)
    lane = lax.broadcasted_iota(jnp.int32, (1, WIDTH), 1)
    scalars = jnp.where(lane == 6, live_count.astype(F32), 0.0)
    for at in range(5):
        scalars = jnp.where(lane == at, totals[at : at + 1], scalars)
    small_rows.append(scalars)
    block_small = jnp.concatenate(small_rows + [jnp.zeros((5, WIDTH), F32)], axis=0)
    pieces = [
        grad0[:, :128],
        grad0[:, 128:],
        grads[3, :, :128],
        grads[3, :, 128:],
        grads[4, :, :128],
        grads[4, :, 128:],
        block_small[:, :128],
        block_small[:, 128:],
        jnp.zeros((PACKED_ROWS - SMALL_ROW - 32, 128), F32),
    ]

    def pack(refs):
        begin = 0
        for piece in pieces:
            rows_left = piece.shape[0]
            done = 0
            while rows_left:
                which, inside = divmod(begin, HALF_ROWS)
                count = min(rows_left, HALF_ROWS - inside)
                refs[which][inside : inside + count, :] = piece[done : done + count]
                begin, done, rows_left = begin + count, done + count, rows_left - count

    @pl.when(core_ref[0] == 0)
    def _():
        pack((kept_ref, given_ref))

    @pl.when(core_ref[0] == 1)
    def _():
        pack((given_ref, kept_ref))


def local_terms(core, counts, offsets, data, in_w, in_b, hid_w, hid_b, out_w, out_b):
    vmem = pl.BlockSpec(memory_space=pltpu.VMEM)
    smem = pl.BlockSpec(memory_space=pltpu.SMEM)
    square = (WIDTH, HALF)
    half = jax.ShapeDtypeStruct((HALF_ROWS, 128), F32)
    return pl.pallas_call(
        step_kernel,
        out_shape=[half, half],
        in_specs=[smem, smem, smem, vmem, vmem, vmem, vmem, vmem, vmem, smem],
        out_specs=[vmem, vmem],
        scratch_shapes=[
            pltpu.VMEM((5, WIDTH, 768), BF16),
            pltpu.VMEM((5, WIDTH, 768), BF16),
            pltpu.VMEM((32, 512), BF16),
            pltpu.VMEM((WIDTH, 32), BF16),
            pltpu.VMEM((8, WIDTH, 128), F32),
            pltpu.VMEM((2, 3, 8, HALF), F32),
            pltpu.VMEM((2, 3, JETS) + square, F32),
            pltpu.VMEM((2, 4) + square, F32),
            pltpu.VMEM((2, 3, JETS) + square, BF16),
            pltpu.VMEM((2, 3, JETS) + square, BF16),
            pltpu.VMEM((2, 3) + square, BF16),
            pltpu.VMEM((2, 3) + square, BF16),
            pltpu.VMEM((2, JETS) + square, F32),
            pltpu.VMEM((2, 2, JETS) + square, BF16),
            pltpu.VMEM((2, 2, JETS) + square, BF16),
            pltpu.VMEM((5, WIDTH, WIDTH), F32),
            pltpu.VMEM((8, WIDTH, 128), F32),
            pltpu.VMEM((32, WIDTH), F32),
            pltpu.VMEM((8, HALF), F32),
        ],
        compiler_params=pltpu.CompilerParams(vmem_limit_bytes=44 * 1024 * 1024),
        name="pinn_step",
    )(core, counts, offsets, data, in_w, in_b.reshape(1, WIDTH), hid_w, hid_b, out_w, out_b)


def unpack_kernel(total_ref, in_w, in_b, hid_w, hid_b, out_w, out_b, means):
    scalars = total_ref[SMALL_ROW + 10 : SMALL_ROW + 11, :]
    scale = 1.0 / scalars[0:1, 6:7]
    for slot in range(3):
        hid_w[slot, :, 0:128] = total_ref[slot * 512 : slot * 512 + 256, :] * scale
        hid_w[slot, :, 128:256] = total_ref[slot * 512 + 256 : slot * 512 + 512, :] * scale

    def rows(first, count):
        at = SMALL_ROW + first
        left = total_ref[at : at + count, :]
        right = total_ref[at + 16 : at + 16 + count, :]
        return jnp.concatenate([left, right], axis=1) * scale

    hid_b[...] = rows(0, 3)
    in_w[...] = rows(3, 3)
    in_b[...] = rows(6, 1)
    out_w[...] = rows(7, 3)
    scaled = scalars * scale
    for i in range(3):
        means[i] = scaled[0, i]
        out_b[i] = scaled[0, 3 + i]


def unpacked(total):
    vmem = pl.BlockSpec(memory_space=pltpu.VMEM)
    shapes = [(3, WIDTH), (1, WIDTH), (3, WIDTH, WIDTH), (3, WIDTH), (3, WIDTH), (3,), (3,)]
    in_w, in_b, hid_w, hid_b, out_w, out_b, means = pl.pallas_call(
        unpack_kernel,
        out_shape=[jax.ShapeDtypeStruct(s, F32) for s in shapes],
        in_specs=[vmem],
        out_specs=[vmem] * 5 + [pl.BlockSpec(memory_space=pltpu.SMEM)] * 2,
        name="unpack",
    )(total)
    return (
        in_w,
        in_b.reshape(WIDTH),
        hid_w,
        hid_b,
        out_w,
        out_b,
        means,
    )


def summed_over_devices(kept, given):
    mine = kept + lax.ppermute(given, NEAR, [(0, 1), (1, 0)])
    members = lax.axis_size(FAR)
    parts = lax.all_to_all(mine.reshape(members, HALF_ROWS // members, 128), FAR, 0, 0, tiled=True)
    own = parts.sum(axis=0)
    spread = jnp.broadcast_to(own[None], (members,) + own.shape)
    gathered = lax.all_to_all(spread, FAR, 0, 0, tiled=True).reshape(HALF_ROWS, 128)
    return lax.all_gather(gathered, NEAR, axis=0, tiled=True)


def shards(
    point_data,
    point_counts,
    point_offsets,
    in_weight,
    input_bias,
    hidden_layer_weight,
    hidden_bias,
    output_weight,
    out_bias,
):
    kept, given = local_terms(
        lax.axis_index(NEAR).reshape(1),
        point_counts,
        point_offsets,
        point_data,
        in_weight,
        input_bias,
        hidden_layer_weight,
        hidden_bias,
        output_weight,
        out_bias,
    )
    return unpacked(summed_over_devices(kept, given))


def solution(mesh):
    torus = Mesh(mesh.devices.reshape(4, 4, 4, 2), PTS)
    placed = (P(None, PTS), P(PTS), P(PTS), P(), P(), P(), P(), P(), P())
    return jax.shard_map(
        shards,
        mesh=torus,
        in_specs=placed,
        out_specs=(P(), P(), P(), P(), P(), P(), P()),
        check_vma=False,
    )
```

```python
import functools

import jax
import jax.numpy as jnp
from jax import lax
from jax.experimental import pallas as pl
from jax.experimental.pallas import tpu as pltpu
from jax.sharding import Mesh
from jax.sharding import PartitionSpec as P

PTS = ("pts_0", "pts_1", "pts_2", "pts_3")
FAR = ("pts_0", "pts_1", "pts_2")
NEAR = "pts_3"

VISCOSITY = 0.2
HALF = 256
WIDTH = 256
ROWS = 16
F32 = jnp.float32
BF16 = jnp.bfloat16
JETS = 4
SMALL_ROW = 3 * 512
PACKED_ROWS = 1664
HALF_ROWS = PACKED_ROWS // 2
TILES = [
    (slice(r * ROWS, (r + 1) * ROWS), slice(c * 128, (c + 1) * 128))
    for r in range(WIDTH // ROWS)
    for c in range(HALF // 128)
]
PAIRS = 2


def split(x):
    high = x.astype(BF16)
    return high, (x - high.astype(F32)).astype(BF16)


def matmul(a, b):
    return lax.dot_general(a, b, (((1,), (0,)), ((), ())), preferred_element_type=F32)


def matmul_nt(a, b):
    return lax.dot_general(a, b, (((1,), (1,)), ((), ())), preferred_element_type=F32)


def step_kernel(
    core_ref,
    counts_ref,
    offsets_ref,
    data_hbm,
    in_w_hbm,
    in_b_hbm,
    hid_w_hbm,
    hid_b_hbm,
    out_w_hbm,
    out_b_hbm,
    kept_ref,
    given_ref,
    data_ref,
    in_w_ref,
    in_b_ref,
    hid_w_ref,
    hid_b_ref,
    out_w_ref,
    out_b_ref,
    copy_sems,
    w_cat,
    wt_cat,
    out_cat,
    outt_cat,
    cols,
    rows_buf,
    z_buf,
    h_buf,
    ah_buf,
    al_buf,
    a0h_buf,
    a0l_buf,
    g_buf,
    dzh_buf,
    dzl_buf,
    grads,
    partial,
    grad_out,
    sums_buf,
):
    copies = [
        pltpu.make_async_copy(source, target, copy_sems.at[i])
        for i, (source, target) in enumerate(
            (
                (in_w_hbm, in_w_ref),
                (hid_w_hbm, hid_w_ref),
                (in_b_hbm, in_b_ref),
                (hid_b_hbm, hid_b_ref),
                (out_w_hbm, out_w_ref),
                (data_hbm, data_ref),
                (out_b_hbm, out_b_ref),
            )
        )
    ]
    for copy in copies:
        copy.start()
    live_start = offsets_ref[0]
    live_count = counts_ref[0]
    first_block = live_start // (2 * HALF * (PAIRS // 2))
    end_block = (live_start + live_count + 2 * HALF - 1) // (2 * HALF)

    grads[...] = jnp.zeros_like(grads)
    partial[...] = jnp.zeros_like(partial)
    sums_buf[...] = jnp.zeros_like(sums_buf)
    grad_out[...] = jnp.zeros_like(grad_out)
    out_cat[...] = jnp.zeros_like(out_cat)
    for copy in copies:
        copy.wait()

    def put_cat(ref, index, value):
        high, low = split(value)
        ref[index, :, 0:256] = high
        ref[index, :, 256:512] = low
        ref[index, :, 512:768] = high

    wx = in_w_ref[0:1, :]
    wy = in_w_ref[1:2, :]
    w0 = hid_w_ref[0]
    for index, w in enumerate((w0, w0 * wx, w0 * wy, hid_w_ref[1], hid_w_ref[2])):
        put_cat(w_cat, index, w)
        put_cat(wt_cat, index, w.T)
    out_high, out_low = split(out_w_ref[...])
    out_cat[0:3, 0:256] = out_high
    out_cat[0:3, 256:512] = out_high
    out_cat[16:19, 0:256] = out_low
    spare = jnp.zeros((5, WIDTH), F32)
    out_rows = jnp.concatenate(
        [out_high.astype(F32), spare, out_low.astype(F32), spare, out_high.astype(F32), spare, jnp.zeros((8, WIDTH), F32)],
        axis=0,
    )
    outt_cat[...] = out_rows.T.astype(BF16)
    rows = jnp.concatenate(
        [
            in_w_ref[...],
            in_b_ref[...],
            hid_b_ref[...],
            wx * wx + wy * wy,
        ],
        axis=0,
    )
    columns = rows.T
    for i in range(8):
        cols[i] = jnp.broadcast_to(columns[:, i : i + 1], (WIDTH, 128))

    def chain(base, at):
        points = data_ref[:, pl.ds(base, HALF)]
        slots = base + lax.broadcasted_iota(jnp.int32, (1, HALF), 1)
        mask = ((slots >= live_start) & (slots < live_start + live_count)).astype(F32)

        def spread(i, row):
            rows_buf[at, i] = jnp.broadcast_to(row, (8, HALF))

        def row(i, lane):
            tile = rows_buf[at, i, :, lane]
            return jnp.concatenate([tile, tile], axis=0)

        for i in range(3):
            spread(i, points[i : i + 1, :])

        def put_split(high_ref, low_ref, where, value):
            high, low = split(value)
            high_ref[where] = high
            low_ref[where] = low

        for r, l in TILES:
            z = cols[0, r] * row(0, l) + cols[1, r] * row(1, l) + cols[2, r] * row(2, l) + cols[3, r]
            h = jnp.tanh(z)
            s = 1.0 - h * h
            h_buf[at, 0, r, l] = h
            d = s * cols[2, r] + (2.0 * VISCOSITY) * (h * s) * cols[7, r]
            for i, a in enumerate((h, s, d)):
                put_split(a0h_buf, a0l_buf, (at, i, r, l), a)
        yield

        def source(layer, jet):
            if layer == 0:
                i = (0, 1, 1, 2)[jet]
                return a0h_buf[at, i], a0l_buf[at, i]
            return ah_buf[at, layer - 1, jet], al_buf[at, layer - 1, jet]

        for layer in range(3):
            for jet in range(JETS):
                high, low = source(layer, jet)
                w = w_cat[(0, 1, 2, 0)[jet]] if layer == 0 else w_cat[layer + 2]
                z_buf[at, layer, jet] = matmul(w, jnp.concatenate([high, high, low], axis=0))
            yield
            for r, l in TILES:
                h = jnp.tanh(z_buf[at, layer, 0, r, l] + cols[4 + layer, r])
                s = 1.0 - h * h
                h_buf[at, layer + 1, r, l] = h
                zx = z_buf[at, layer, 1, r, l]
                zy = z_buf[at, layer, 2, r, l]
                d = s * z_buf[at, layer, 3, r, l] + (2.0 * VISCOSITY) * (h * s) * (
                    zx * zx + zy * zy
                )
                for jet, a in enumerate((h, s * zx, s * zy, d)):
                    put_split(ah_buf, al_buf, (at, layer, jet, r, l), a)
            yield

        outs = []
        for jet in range(JETS):
            high, low = source(3, jet)
            both = matmul(out_cat[...], jnp.concatenate([high, low], axis=0))
            outs.append(both[0:8] + both[16:24])
        u = outs[0][0:1] + out_b_ref[0]
        v = outs[0][1:2] + out_b_ref[1]
        u_x, v_x, p_x = outs[1][0:1], outs[1][1:2], outs[1][2:3]
        u_y, v_y, p_y = outs[2][0:1], outs[2][1:2], outs[2][2:3]
        u_d, v_d = outs[3][0:1], outs[3][1:2]
        cont = mask * (u_x + v_y)
        mom_x = mask * (u_d + u * u_x + v * u_y + p_x - points[3:4, :])
        mom_y = mask * (v_d + u * v_x + v * v_y + p_y - points[4:5, :])
        gc = 4.0 * cont
        gx = 2.0 * mom_x
        gy = 2.0 * mom_y
        du = gx * u_x + gy * v_x
        dv = gx * u_y + gy * v_y
        nothing = jnp.zeros_like(gx)
        cotangents = [
            jnp.concatenate([a, b, c] + [nothing] * 5, axis=0)
            for a, b, c in (
                (du, dv, nothing),
                (gc + gx * u, gy * u, gx),
                (gx * v, gc + gy * v, gy),
                (gx, gy, nothing),
            )
        ]
        sums_buf[0:1, :] += cont * cont
        sums_buf[1:2, :] += mom_x * mom_x
        sums_buf[2:3, :] += mom_y * mom_y
        sums_buf[3:4, :] += du
        sums_buf[4:5, :] += dv
        left, right = [], []
        for jet, value in enumerate(cotangents):
            high = value.astype(BF16).astype(F32)
            low = value - high
            g_buf[at, jet] = matmul(
                outt_cat[...],
                jnp.concatenate([high, high, low, jnp.zeros_like(low)], axis=0).astype(BF16),
            )
            pad = jnp.zeros_like(high)
            both = jnp.concatenate([high, pad, low, pad], axis=0).astype(BF16)
            alone = jnp.concatenate([high, pad, pad, pad], axis=0).astype(BF16)
            a_high, a_low = source(3, jet)
            left += [both, alone]
            right += [a_high, a_low]
        grad_out[...] += matmul_nt(jnp.concatenate(left, axis=1), jnp.concatenate(right, axis=1))
        yield

        def activation_back(a, r, l):
            h = h_buf[at, a, r, l]
            s = 1.0 - h * h
            zx = z_buf[at, a - 1, 1, r, l]
            zy = z_buf[at, a - 1, 2, r, l]
            zd = z_buf[at, a - 1, 3, r, l]
            square = zx * zx + zy * zy
            q = (2.0 * VISCOSITY) * (h * s)
            g0, g1, g2, g3 = [g_buf[at, jet, r, l] for jet in range(JETS)]
            qg = 2.0 * (q * g3)
            d_s = zx * g1 + zy * g2 + zd * g3
            d_q = square * g3
            d0 = s * (g0 - 2.0 * (h * d_s) + (6.0 * VISCOSITY * s - 4.0 * VISCOSITY) * d_q)
            d1 = s * g1 + qg * zx
            d2 = s * g2 + qg * zy
            partial[a - 1, r] += d0
            for jet, d in enumerate((d0, d1, d2, s * g3)):
                put_split(dzh_buf, dzl_buf, (at, a % 2, jet, r, l), d)

        for r, l in TILES:
            activation_back(3, r, l)
        yield

        for layer in (2, 1):
            up = (layer + 1) % 2
            for jet in range(JETS):
                high = dzh_buf[at, up, jet]
                g_buf[at, jet] = matmul(
                    wt_cat[layer + 2],
                    jnp.concatenate([high, high, dzl_buf[at, up, jet]], axis=0),
                )
            left, right = [], []
            for jet in range(JETS):
                high = dzh_buf[at, up, jet]
                left += [high, dzl_buf[at, up, jet], high]
                a_high, a_low = source(layer, jet)
                right += [a_high, a_high, a_low]
            grads[layer + 2] += matmul_nt(
                jnp.concatenate(left, axis=1), jnp.concatenate(right, axis=1)
            )
            yield
            for r, l in TILES:
                activation_back(layer, r, l)
            yield

        def stacked(jet):
            high = dzh_buf[at, 1, jet]
            return [high, high, dzl_buf[at, 1, jet]]

        g_buf[at, 0] = matmul(wt_cat[0], jnp.concatenate(stacked(0), axis=0))
        g_buf[at, 1] = matmul(
            jnp.concatenate([wt_cat[1], wt_cat[2]], axis=1),
            jnp.concatenate(stacked(1) + stacked(2), axis=0),
        )
        g_buf[at, 2] = matmul(wt_cat[0], jnp.concatenate(stacked(3), axis=0))
        for index, jets in enumerate(((0, 3), (1,), (2,))):
            left, right = [], []
            for jet in jets:
                high = dzh_buf[at, 1, jet]
                left += [high, dzl_buf[at, 1, jet], high]
                a_high, a_low = source(0, jet)
                right += [a_high, a_high, a_low]
            grads[index] += matmul_nt(
                jnp.concatenate(left, axis=1), jnp.concatenate(right, axis=1)
            )
        yield
        for r, l in TILES:
            h = h_buf[at, 0, r, l]
            s = 1.0 - h * h
            g3 = g_buf[at, 2, r, l]
            d_s = g_buf[at, 1, r, l] + cols[2, r] * g3
            d_q = cols[7, r] * g3
            d = s * (
                g_buf[at, 0, r, l]
                - 2.0 * (h * d_s)
                + (6.0 * VISCOSITY * s - 4.0 * VISCOSITY) * d_q
            )
            partial[3, r] += d * row(0, l)
            partial[4, r] += d * row(1, l)
            partial[5, r] += d * row(2, l) + s * g3
            partial[6, r] += d
            partial[7, r] += (2.0 * VISCOSITY) * (h * s) * g3
        yield

    def run(chains):
        queues = [[chains[i] for i in range(k, len(chains), 2)] for k in range(2)]
        started = False
        while any(queues):
            for k, queue in enumerate(queues):
                if k == 1 and not started:
                    started = True
                    continue
                while queue:
                    try:
                        next(queue[0])
                        break
                    except StopIteration:
                        queue.pop(0)

    if PAIRS == 4:
        run([chain(i * HALF, i % 2) for i in range(4)])
    else:

        def block(index, carry):
            base = pl.multiple_of(index * (2 * HALF), 2 * HALF)
            run([chain(pl.multiple_of(base + i * HALF, HALF), i) for i in range(2)])
            return carry

        lax.fori_loop(first_block, end_block, block, 0)

    wt = in_w_ref[2:3, :]
    grad0 = grads[0] + grads[1] * wx + grads[2] * wy
    direct = [
        jnp.sum(w0 * grads[1], axis=0, keepdims=True),
        jnp.sum(w0 * grads[2], axis=0, keepdims=True),
    ]
    lanes = lax.broadcasted_iota(jnp.int32, (WIDTH, 128), 1)
    placed = jnp.zeros((WIDTH, 128), F32)
    for i in range(8):
        placed = jnp.where(lanes == i, jnp.sum(partial[i], axis=1, keepdims=True), placed)
    small = placed.T[0:16]
    small_rows = [small[i : i + 1] for i in range(7)]
    small_rows.append(grad_out[0:3, :] + grad_out[16:19, :])
    by_square = 2.0 * small[7:8]
    small_rows[3] = small_rows[3] + direct[0] + by_square * wx
    small_rows[4] = small_rows[4] + direct[1] + by_square * wy
    totals = jnp.sum(sums_buf[...], axis=1, keepdims=True)
    lane = lax.broadcasted_iota(jnp.int32, (1, WIDTH), 1)
    scalars = jnp.where(lane == 6, live_count.astype(F32), 0.0)
    for at in range(5):
        scalars = jnp.where(lane == at, totals[at : at + 1], scalars)
    small_rows.append(scalars)
    block_small = jnp.concatenate(small_rows + [jnp.zeros((5, WIDTH), F32)], axis=0)
    pieces = [
        grad0[:, :128],
        grad0[:, 128:],
        grads[3, :, :128],
        grads[3, :, 128:],
        grads[4, :, :128],
        grads[4, :, 128:],
        block_small[:, :128],
        block_small[:, 128:],
        jnp.zeros((PACKED_ROWS - SMALL_ROW - 32, 128), F32),
    ]

    def pack(refs):
        begin = 0
        for piece in pieces:
            rows_left = piece.shape[0]
            done = 0
            while rows_left:
                which, inside = divmod(begin, HALF_ROWS)
                count = min(rows_left, HALF_ROWS - inside)
                refs[which][inside : inside + count, :] = piece[done : done + count]
                begin, done, rows_left = begin + count, done + count, rows_left - count

    @pl.when(core_ref[0] == 0)
    def _():
        pack((kept_ref, given_ref))

    @pl.when(core_ref[0] == 1)
    def _():
        pack((given_ref, kept_ref))


def local_terms(core, counts, offsets, data, in_w, in_b, hid_w, hid_b, out_w, out_b):
    vmem = pl.BlockSpec(memory_space=pltpu.VMEM)
    smem = pl.BlockSpec(memory_space=pltpu.SMEM)
    square = (WIDTH, HALF)
    half = jax.ShapeDtypeStruct((HALF_ROWS, 128), F32)
    inputs = [
        pltpu.with_memory_space_constraint(x, pltpu.HBM)
        for x in (data, in_w, in_b.reshape(1, WIDTH), hid_w, hid_b, out_w, out_b)
    ]
    return pl.pallas_call(
        step_kernel,
        out_shape=[half, half],
        in_specs=[smem] * 3 + [pl.BlockSpec(memory_space=pltpu.HBM)] * 7,
        out_specs=[vmem, vmem],
        scratch_shapes=[
            pltpu.VMEM(data.shape, F32),
            pltpu.VMEM((3, WIDTH), F32),
            pltpu.VMEM((1, WIDTH), F32),
            pltpu.VMEM((3, WIDTH, WIDTH), F32),
            pltpu.VMEM((3, WIDTH), F32),
            pltpu.VMEM((3, WIDTH), F32),
            pltpu.SMEM((3,), F32),
            pltpu.SemaphoreType.DMA((7,)),
            pltpu.VMEM((5, WIDTH, 768), BF16),
            pltpu.VMEM((5, WIDTH, 768), BF16),
            pltpu.VMEM((32, 512), BF16),
            pltpu.VMEM((WIDTH, 32), BF16),
            pltpu.VMEM((8, WIDTH, 128), F32),
            pltpu.VMEM((2, 3, 8, HALF), F32),
            pltpu.VMEM((2, 3, JETS) + square, F32),
            pltpu.VMEM((2, 4) + square, F32),
            pltpu.VMEM((2, 3, JETS) + square, BF16),
            pltpu.VMEM((2, 3, JETS) + square, BF16),
            pltpu.VMEM((2, 3) + square, BF16),
            pltpu.VMEM((2, 3) + square, BF16),
            pltpu.VMEM((2, JETS) + square, F32),
            pltpu.VMEM((2, 2, JETS) + square, BF16),
            pltpu.VMEM((2, 2, JETS) + square, BF16),
            pltpu.VMEM((5, WIDTH, WIDTH), F32),
            pltpu.VMEM((8, WIDTH, 128), F32),
            pltpu.VMEM((32, WIDTH), F32),
            pltpu.VMEM((8, HALF), F32),
        ],
        compiler_params=pltpu.CompilerParams(vmem_limit_bytes=44 * 1024 * 1024),
        name="pinn_step",
    )(core, counts, offsets, *inputs)


def unpack_kernel(
    core_ref, own_ref, other_ref, in_w, in_b, hid_w_hbm, hid_b, out_w, out_b, means, hid_w, copy_sems
):
    def fill(halves):
        def rows(begin, count):
            parts = []
            while count:
                which, inside = divmod(begin, HALF_ROWS)
                taken = min(count, HALF_ROWS - inside)
                parts.append(halves[which][inside : inside + taken, :])
                begin, count = begin + taken, count - taken
            return parts[0] if len(parts) == 1 else jnp.concatenate(parts, axis=0)

        small = jnp.concatenate([rows(SMALL_ROW, 16), rows(SMALL_ROW + 16, 16)], axis=1)
        scalars = small[10:11]
        scale = 1.0 / scalars[0:1, 6:7]
        copies = []
        for slot in range(3):
            hid_w[slot, :, 0:128] = rows(slot * 512, 256) * scale
            hid_w[slot, :, 128:256] = rows(slot * 512 + 256, 256) * scale
            copies.append(
                pltpu.make_async_copy(hid_w.at[slot], hid_w_hbm.at[slot], copy_sems.at[slot])
            )
            copies[-1].start()
        scaled = small * scale
        hid_b[...] = scaled[0:3]
        in_w[...] = scaled[3:6]
        in_b[...] = scaled[6:7]
        out_w[...] = scaled[7:10]
        for i in range(3):
            means[i] = scaled[10, i]
            out_b[i] = scaled[10, 3 + i]
        for copy in copies:
            copy.wait()

    @pl.when(core_ref[0] == 0)
    def _():
        fill((own_ref, other_ref))

    @pl.when(core_ref[0] == 1)
    def _():
        fill((other_ref, own_ref))


def unpacked(core, own, other):
    vmem = pl.BlockSpec(memory_space=pltpu.VMEM)
    smem = pl.BlockSpec(memory_space=pltpu.SMEM)
    shapes = [(3, WIDTH), (1, WIDTH), (3, WIDTH, WIDTH), (3, WIDTH), (3, WIDTH), (3,), (3,)]
    in_w, in_b, hid_w, hid_b, out_w, out_b, means = pl.pallas_call(
        unpack_kernel,
        out_shape=[jax.ShapeDtypeStruct(s, F32) for s in shapes],
        in_specs=[smem, vmem, vmem],
        out_specs=[vmem, vmem, pl.BlockSpec(memory_space=pltpu.HBM), vmem, vmem, smem, smem],
        scratch_shapes=[
            pltpu.VMEM((3, WIDTH, WIDTH), F32),
            pltpu.SemaphoreType.DMA((3,)),
        ],
        compiler_params=pltpu.CompilerParams(vmem_limit_bytes=8 * 1024 * 1024),
        name="unpack",
    )(core, own, other)
    return in_w, in_b.reshape(WIDTH), hid_w, hid_b, out_w, out_b, means


def summed_over_devices(kept, given):
    mine = kept + lax.ppermute(given, NEAR, [(0, 1), (1, 0)])
    members = lax.axis_size(FAR)
    parts = lax.all_to_all(mine.reshape(members, HALF_ROWS // members, 128), FAR, 0, 0, tiled=True)
    own = parts.sum(axis=0)
    spread = jnp.broadcast_to(own[None], (members,) + own.shape)
    own = lax.all_to_all(spread, FAR, 0, 0, tiled=True).reshape(HALF_ROWS, 128)
    return own, lax.ppermute(own, NEAR, [(0, 1), (1, 0)])


def shards(
    point_data,
    point_counts,
    point_offsets,
    in_weight,
    input_bias,
    hidden_layer_weight,
    hidden_bias,
    output_weight,
    out_bias,
):
    core = lax.axis_index(NEAR).reshape(1)
    kept, given = local_terms(
        core,
        point_counts,
        point_offsets,
        point_data,
        in_weight,
        input_bias,
        hidden_layer_weight,
        hidden_bias,
        output_weight,
        out_bias,
    )
    return unpacked(core, *summed_over_devices(kept, given))


def solution(mesh):
    torus = Mesh(mesh.devices.reshape(4, 4, 4, 2), PTS)
    placed = (P(None, PTS), P(PTS), P(PTS), P(), P(), P(), P(), P(), P())
    return jax.shard_map(
        shards,
        mesh=torus,
        in_specs=placed,
        out_specs=(P(), P(), P(), P(), P(), P(), P()),
        check_vma=False,
    )
```

```python
import functools

import jax
import jax.numpy as jnp
from jax import lax
from jax.experimental import pallas as pl
from jax.experimental.pallas import tpu as pltpu
from jax.sharding import Mesh
from jax.sharding import PartitionSpec as P

PTS = ("pts_0", "pts_1", "pts_2", "pts_3")
FAR = ("pts_0", "pts_1", "pts_2")
NEAR = "pts_3"

VISCOSITY = 0.2
HALF = 256
WIDTH = 256
ROWS = 16
F32 = jnp.float32
BF16 = jnp.bfloat16
JETS = 4
HALF_ROWS = 832
PIECES = (
    ((0, 0, 0, 256, 0), (0, 1, 0, 256, 256), (1, 0, 0, 256, 512), (1, 1, 0, 48, 768)),
    ((1, 1, 48, 208, 0), (2, 0, 0, 256, 208), (2, 1, 0, 256, 464)),
)
SMALL_ROW = 720
COUNT_ROWS = (816, 752)
TILES = [
    (slice(r * ROWS, (r + 1) * ROWS), slice(c * 128, (c + 1) * 128))
    for r in range(WIDTH // ROWS)
    for c in range(HALF // 128)
]
OFFSET = 3


def split(x):
    high = x.astype(BF16)
    return high, (x - high.astype(F32)).astype(BF16)


def matmul(a, b):
    return lax.dot_general(a, b, (((1,), (0,)), ((), ())), preferred_element_type=F32)


def matmul_nt(a, b):
    return lax.dot_general(a, b, (((1,), (1,)), ((), ())), preferred_element_type=F32)


def step_kernel(
    counts_ref,
    offsets_ref,
    data_hbm,
    in_w_hbm,
    in_b_hbm,
    hid_w_hbm,
    hid_b_hbm,
    out_w_hbm,
    out_b_hbm,
    kept_ref,
    given_ref,
    data_ref,
    in_w_ref,
    in_b_ref,
    hid_w_ref,
    hid_b_ref,
    out_w_ref,
    out_b_ref,
    copy_sems,
    w_cat,
    wt_cat,
    out_cat,
    outt_cat,
    cols,
    rows_buf,
    z_buf,
    h_buf,
    ah_buf,
    al_buf,
    a0h_buf,
    a0l_buf,
    g_buf,
    dzh_buf,
    dzl_buf,
    grads,
    partial,
    grad_out,
    sums_buf,
):
    copies = [
        pltpu.make_async_copy(source, target, copy_sems.at[i])
        for i, (source, target) in enumerate(
            (
                (in_w_hbm, in_w_ref),
                (in_b_hbm, in_b_ref),
                (hid_b_hbm, hid_b_ref),
                (out_w_hbm, out_w_ref),
                (hid_w_hbm, hid_w_ref),
                (data_hbm, data_ref),
                (out_b_hbm, out_b_ref),
            )
        )
    ]
    for copy in copies:
        copy.start()
    core = lax.axis_index(NEAR)
    grads[...] = jnp.zeros_like(grads)
    partial[...] = jnp.zeros_like(partial)
    sums_buf[...] = jnp.zeros_like(sums_buf)
    grad_out[...] = jnp.zeros_like(grad_out)
    out_cat[...] = jnp.zeros_like(out_cat)
    for copy in copies[:4]:
        copy.wait()

    wx = in_w_ref[0:1, :]
    wy = in_w_ref[1:2, :]
    rows = jnp.concatenate(
        [
            in_w_ref[...],
            in_b_ref[...],
            hid_b_ref[...],
            wx * wx + wy * wy,
        ],
        axis=0,
    )
    columns = rows.T
    for i in range(8):
        cols[i] = jnp.broadcast_to(columns[:, i : i + 1], (WIDTH, 128))

    for copy in copies[4:]:
        copy.wait()
    live_start = offsets_ref[0]
    live_count = counts_ref[0]
    first_block = live_start // (2 * HALF)
    end_block = (live_start + live_count + 2 * HALF - 1) // (2 * HALF)

    def put_cat(ref, index, value):
        high, low = split(value)
        ref[index, :, 0:256] = high
        ref[index, :, 256:512] = low
        ref[index, :, 512:768] = high

    w0 = hid_w_ref[0]
    for index, w in enumerate((w0, w0 * wx, w0 * wy, hid_w_ref[1], hid_w_ref[2])):
        put_cat(w_cat, index, w)
        put_cat(wt_cat, index, w.T)
    out_high, out_low = split(out_w_ref[...])
    out_cat[0:3, 0:256] = out_high
    out_cat[0:3, 256:512] = out_high
    out_cat[16:19, 0:256] = out_low
    spare = jnp.zeros((5, WIDTH), F32)
    out_rows = jnp.concatenate(
        [out_high.astype(F32), spare, out_low.astype(F32), spare, out_high.astype(F32), spare, jnp.zeros((8, WIDTH), F32)],
        axis=0,
    )
    outt_cat[...] = out_rows.T.astype(BF16)
    def chain(base, at):
        points = data_ref[:, pl.ds(base, HALF)]
        slots = base + lax.broadcasted_iota(jnp.int32, (1, HALF), 1)
        mask = ((slots >= live_start) & (slots < live_start + live_count)).astype(F32)

        def spread(i, row):
            rows_buf[at, i] = jnp.broadcast_to(row, (8, HALF))

        def row(i, lane):
            tile = rows_buf[at, i, :, lane]
            return jnp.concatenate([tile, tile], axis=0)

        for i in range(3):
            spread(i, points[i : i + 1, :])

        def put_split(high_ref, low_ref, where, value):
            high, low = split(value)
            high_ref[where] = high
            low_ref[where] = low

        for r, l in TILES:
            z = cols[0, r] * row(0, l) + cols[1, r] * row(1, l) + cols[2, r] * row(2, l) + cols[3, r]
            h = jnp.tanh(z)
            s = 1.0 - h * h
            h_buf[at, 0, r, l] = h
            d = s * cols[2, r] + (2.0 * VISCOSITY) * (h * s) * cols[7, r]
            for i, a in enumerate((h, s, d)):
                put_split(a0h_buf, a0l_buf, (at, i, r, l), a)
        yield

        def source(layer, jet):
            if layer == 0:
                i = (0, 1, 1, 2)[jet]
                return a0h_buf[at, i], a0l_buf[at, i]
            return ah_buf[at, layer - 1, jet], al_buf[at, layer - 1, jet]

        for layer in range(3):
            for jet in range(JETS):
                high, low = source(layer, jet)
                w = w_cat[(0, 1, 2, 0)[jet]] if layer == 0 else w_cat[layer + 2]
                z_buf[at, layer, jet] = matmul(w, jnp.concatenate([high, high, low], axis=0))
            yield
            for r, l in TILES:
                h = jnp.tanh(z_buf[at, layer, 0, r, l] + cols[4 + layer, r])
                s = 1.0 - h * h
                h_buf[at, layer + 1, r, l] = h
                zx = z_buf[at, layer, 1, r, l]
                zy = z_buf[at, layer, 2, r, l]
                d = s * z_buf[at, layer, 3, r, l] + (2.0 * VISCOSITY) * (h * s) * (
                    zx * zx + zy * zy
                )
                for jet, a in enumerate((h, s * zx, s * zy, d)):
                    put_split(ah_buf, al_buf, (at, layer, jet, r, l), a)
            yield

        outs = []
        for jet in range(JETS):
            high, low = source(3, jet)
            both = matmul(out_cat[...], jnp.concatenate([high, low], axis=0))
            outs.append(both[0:8] + both[16:24])
        u = outs[0][0:1] + out_b_ref[0]
        v = outs[0][1:2] + out_b_ref[1]
        u_x, v_x, p_x = outs[1][0:1], outs[1][1:2], outs[1][2:3]
        u_y, v_y, p_y = outs[2][0:1], outs[2][1:2], outs[2][2:3]
        u_d, v_d = outs[3][0:1], outs[3][1:2]
        cont = mask * (u_x + v_y)
        mom_x = mask * (u_d + u * u_x + v * u_y + p_x - points[3:4, :])
        mom_y = mask * (v_d + u * v_x + v * v_y + p_y - points[4:5, :])
        gc = 4.0 * cont
        gx = 2.0 * mom_x
        gy = 2.0 * mom_y
        du = gx * u_x + gy * v_x
        dv = gx * u_y + gy * v_y
        nothing = jnp.zeros_like(gx)
        cotangents = [
            jnp.concatenate([a, b, c] + [nothing] * 5, axis=0)
            for a, b, c in (
                (du, dv, nothing),
                (gc + gx * u, gy * u, gx),
                (gx * v, gc + gy * v, gy),
                (gx, gy, nothing),
            )
        ]
        sums_buf[0:1, :] += cont * cont
        sums_buf[1:2, :] += mom_x * mom_x
        sums_buf[2:3, :] += mom_y * mom_y
        sums_buf[3:4, :] += du
        sums_buf[4:5, :] += dv
        left, right = [], []
        for jet, value in enumerate(cotangents):
            high = value.astype(BF16).astype(F32)
            low = value - high
            g_buf[at, jet] = matmul(
                outt_cat[...],
                jnp.concatenate([high, high, low, jnp.zeros_like(low)], axis=0).astype(BF16),
            )
            pad = jnp.zeros_like(high)
            both = jnp.concatenate([high, pad, low, pad], axis=0).astype(BF16)
            alone = jnp.concatenate([high, pad, pad, pad], axis=0).astype(BF16)
            a_high, a_low = source(3, jet)
            left += [both, alone]
            right += [a_high, a_low]
        grad_out[...] += matmul_nt(jnp.concatenate(left, axis=1), jnp.concatenate(right, axis=1))
        yield

        def activation_back(a, r, l):
            h = h_buf[at, a, r, l]
            s = 1.0 - h * h
            zx = z_buf[at, a - 1, 1, r, l]
            zy = z_buf[at, a - 1, 2, r, l]
            zd = z_buf[at, a - 1, 3, r, l]
            square = zx * zx + zy * zy
            g0, g1, g2, g3 = [g_buf[at, jet, r, l] for jet in range(JETS)]
            k = ((4.0 * VISCOSITY) * h) * g3
            d_s = zx * g1 + zy * g2 + zd * g3
            d_q = square * g3
            d0 = s * (g0 - 2.0 * (h * d_s) + (6.0 * VISCOSITY * s - 4.0 * VISCOSITY) * d_q)
            d1 = s * (g1 + k * zx)
            d2 = s * (g2 + k * zy)
            partial[a - 1, r] += d0
            for jet, d in enumerate((d0, d1, d2, s * g3)):
                put_split(dzh_buf, dzl_buf, (at, a % 2, jet, r, l), d)

        for r, l in TILES:
            activation_back(3, r, l)
        yield

        for layer in (2, 1):
            up = (layer + 1) % 2
            for jet in range(JETS):
                high = dzh_buf[at, up, jet]
                g_buf[at, jet] = matmul(
                    wt_cat[layer + 2],
                    jnp.concatenate([high, high, dzl_buf[at, up, jet]], axis=0),
                )
            left, right = [], []
            for jet in range(JETS):
                high = dzh_buf[at, up, jet]
                left += [high, dzl_buf[at, up, jet], high]
                a_high, a_low = source(layer, jet)
                right += [a_high, a_high, a_low]
            grads[layer + 2] += matmul_nt(
                jnp.concatenate(left, axis=1), jnp.concatenate(right, axis=1)
            )
            yield
            for r, l in TILES:
                activation_back(layer, r, l)
            yield

        def stacked(jet):
            high = dzh_buf[at, 1, jet]
            return [high, high, dzl_buf[at, 1, jet]]

        g_buf[at, 0] = matmul(wt_cat[0], jnp.concatenate(stacked(0), axis=0))
        g_buf[at, 1] = matmul(
            jnp.concatenate([wt_cat[1], wt_cat[2]], axis=1),
            jnp.concatenate(stacked(1) + stacked(2), axis=0),
        )
        g_buf[at, 2] = matmul(wt_cat[0], jnp.concatenate(stacked(3), axis=0))
        for index, jets in enumerate(((0, 3), (1,), (2,))):
            left, right = [], []
            for jet in jets:
                high = dzh_buf[at, 1, jet]
                left += [high, dzl_buf[at, 1, jet], high]
                a_high, a_low = source(0, jet)
                right += [a_high, a_high, a_low]
            grads[index] += matmul_nt(
                jnp.concatenate(left, axis=1), jnp.concatenate(right, axis=1)
            )
        yield
        for r, l in TILES:
            h = h_buf[at, 0, r, l]
            s = 1.0 - h * h
            g3 = g_buf[at, 2, r, l]
            d_s = g_buf[at, 1, r, l] + cols[2, r] * g3
            d_q = cols[7, r] * g3
            d = s * (
                g_buf[at, 0, r, l]
                - 2.0 * (h * d_s)
                + (6.0 * VISCOSITY * s - 4.0 * VISCOSITY) * d_q
            )
            partial[3, r] += d * row(0, l)
            partial[4, r] += d * row(1, l)
            partial[5, r] += d * row(2, l) + s * g3
            partial[6, r] += d
            partial[7, r] += (2.0 * VISCOSITY) * (h * s) * g3
        yield

    def run(chains):
        waiting = list(chains)
        at = 0
        while waiting:
            for k, stages in enumerate(chains):
                if stages in waiting and (k == 0 or at >= OFFSET):
                    if next(stages, "end") == "end":
                        waiting.remove(stages)
            at += 1

    def block(index, carry):
        base = pl.multiple_of(index * (2 * HALF), 2 * HALF)
        run([chain(pl.multiple_of(base + i * HALF, HALF), i) for i in range(2)])
        return carry

    lax.fori_loop(first_block, end_block, block, 0)

    wt = in_w_ref[2:3, :]
    grad0 = grads[0] + grads[1] * wx + grads[2] * wy
    direct = [
        jnp.sum(w0 * grads[1], axis=0, keepdims=True),
        jnp.sum(w0 * grads[2], axis=0, keepdims=True),
    ]
    lanes = lax.broadcasted_iota(jnp.int32, (WIDTH, 128), 1)
    placed = jnp.zeros((WIDTH, 128), F32)
    for i in range(8):
        placed = jnp.where(lanes == i, jnp.sum(partial[i], axis=1, keepdims=True), placed)
    small = placed.T[0:16]
    small_rows = [small[i : i + 1] for i in range(7)]
    small_rows.append(grad_out[0:3, :] + grad_out[16:19, :])
    by_square = 2.0 * small[7:8]
    small_rows[3] = small_rows[3] + direct[0] + by_square * wx
    small_rows[4] = small_rows[4] + direct[1] + by_square * wy
    totals = jnp.sum(sums_buf[...], axis=1, keepdims=True)
    lane = lax.broadcasted_iota(jnp.int32, (1, WIDTH), 1)
    scalars = jnp.zeros((1, WIDTH), F32)
    for at in range(5):
        scalars = jnp.where(lane == at, totals[at : at + 1], scalars)
    small_rows.append(scalars)
    block_small = jnp.concatenate(small_rows + [jnp.zeros((5, WIDTH), F32)], axis=0)
    count_rows = jnp.broadcast_to(live_count.astype(F32), (8, 128))

    def pack(refs):
        for ref, pieces, count_row in zip(refs, PIECES, COUNT_ROWS):
            for layer, side, first, rows, at in pieces:
                columns = slice(side * 128, side * 128 + 128)
                if layer == 0:
                    value = grad0[first : first + rows, columns]
                else:
                    value = grads[layer + 2, first : first + rows, columns]
                ref[at : at + rows, :] = value
            ref[count_row : count_row + 8, :] = count_rows
            ref[count_row + 8 :, :] = jnp.zeros((HALF_ROWS - count_row - 8, 128), F32)
        refs[1][SMALL_ROW : SMALL_ROW + 16, :] = block_small[:, :128]
        refs[1][SMALL_ROW + 16 : SMALL_ROW + 32, :] = block_small[:, 128:]

    @pl.when(core == 0)
    def _():
        pack((kept_ref, given_ref))

    @pl.when(core == 1)
    def _():
        pack((given_ref, kept_ref))


def local_terms(counts, offsets, data, in_w, in_b, hid_w, hid_b, out_w, out_b):
    vmem = pl.BlockSpec(memory_space=pltpu.VMEM)
    square = (WIDTH, HALF)
    half = jax.ShapeDtypeStruct((HALF_ROWS, 128), F32)
    inputs = [
        pltpu.with_memory_space_constraint(x, pltpu.HBM)
        for x in (data, in_w, in_b.reshape(1, WIDTH), hid_w, hid_b, out_w, out_b)
    ]
    return pl.pallas_call(
        step_kernel,
        out_shape=[half, half],
        in_specs=[pl.BlockSpec(memory_space=pltpu.SMEM)] * 2
        + [pl.BlockSpec(memory_space=pltpu.HBM)] * 7,
        out_specs=[vmem, vmem],
        scratch_shapes=[
            pltpu.VMEM(data.shape, F32),
            pltpu.VMEM((3, WIDTH), F32),
            pltpu.VMEM((1, WIDTH), F32),
            pltpu.VMEM((3, WIDTH, WIDTH), F32),
            pltpu.VMEM((3, WIDTH), F32),
            pltpu.VMEM((3, WIDTH), F32),
            pltpu.SMEM((3,), F32),
            pltpu.SemaphoreType.DMA((7,)),
            pltpu.VMEM((5, WIDTH, 768), BF16),
            pltpu.VMEM((5, WIDTH, 768), BF16),
            pltpu.VMEM((32, 512), BF16),
            pltpu.VMEM((WIDTH, 32), BF16),
            pltpu.VMEM((8, WIDTH, 128), F32),
            pltpu.VMEM((2, 3, 8, HALF), F32),
            pltpu.VMEM((2, 3, JETS) + square, F32),
            pltpu.VMEM((2, 4) + square, F32),
            pltpu.VMEM((2, 3, JETS) + square, BF16),
            pltpu.VMEM((2, 3, JETS) + square, BF16),
            pltpu.VMEM((2, 3) + square, BF16),
            pltpu.VMEM((2, 3) + square, BF16),
            pltpu.VMEM((2, JETS) + square, F32),
            pltpu.VMEM((2, 2, JETS) + square, BF16),
            pltpu.VMEM((2, 2, JETS) + square, BF16),
            pltpu.VMEM((5, WIDTH, WIDTH), F32),
            pltpu.VMEM((8, WIDTH, 128), F32),
            pltpu.VMEM((32, WIDTH), F32),
            pltpu.VMEM((8, HALF), F32),
        ],
        compiler_params=pltpu.CompilerParams(vmem_limit_bytes=44 * 1024 * 1024),
        name="pinn_step",
    )(counts, offsets, *inputs)


def put_half(ref, half, hid_w_hbm, buffer, copy_sems):
    scale = 1.0 / ref[COUNT_ROWS[half] : COUNT_ROWS[half] + 1, :]
    copies = []
    for i, (layer, side, first, rows, at) in enumerate(PIECES[half]):
        buffer[at : at + rows, :] = ref[at : at + rows, :] * scale
        copies.append(
            pltpu.make_async_copy(
                buffer.at[pl.ds(at, rows), :],
                hid_w_hbm.at[layer, pl.ds(first, rows), pl.ds(side * 128, 128)],
                copy_sems.at[i],
            )
        )
        copies[-1].start()
    return copies


def own_kernel(own_ref, hid_w_hbm, buffer, copy_sems):
    core = lax.axis_index(NEAR)
    for half in range(2):

        @pl.when(core == half)
        def _():
            for copy in put_half(own_ref, half, hid_w_hbm, buffer, copy_sems):
                copy.wait()


def other_kernel(
    own_ref, other_ref, _, hid_w_hbm, in_w, in_b, hid_b, out_w, out_b, means, buffer, copy_sems
):
    core = lax.axis_index(NEAR)

    def small(ref):
        scale = 1.0 / ref[COUNT_ROWS[1] : COUNT_ROWS[1] + 1, :]
        left = ref[SMALL_ROW : SMALL_ROW + 16, :] * scale
        right = ref[SMALL_ROW + 16 : SMALL_ROW + 32, :] * scale
        rows = jnp.concatenate([left, right], axis=1)
        hid_b[...] = rows[0:3]
        in_w[...] = rows[3:6]
        in_b[...] = rows[6:7]
        out_w[...] = rows[7:10]
        for i in range(3):
            means[i] = left[10, i]
            out_b[i] = left[10, 3 + i]

    for half in range(2):

        @pl.when(core == 1 - half)
        def _():
            copies = put_half(other_ref, half, hid_w_hbm, buffer, copy_sems)
            small((own_ref, other_ref)[half])
            for copy in copies:
                copy.wait()


def unpacked(own, other):
    vmem = pl.BlockSpec(memory_space=pltpu.VMEM)
    smem = pl.BlockSpec(memory_space=pltpu.SMEM)
    hbm = pl.BlockSpec(memory_space=pltpu.HBM)
    whole = jax.ShapeDtypeStruct((3, WIDTH, WIDTH), F32)
    scratch = [pltpu.VMEM((HALF_ROWS, 128), F32), pltpu.SemaphoreType.DMA((4,))]
    params = pltpu.CompilerParams(vmem_limit_bytes=8 * 1024 * 1024)
    half_done = pl.pallas_call(
        own_kernel,
        out_shape=whole,
        in_specs=[vmem],
        out_specs=hbm,
        scratch_shapes=scratch,
        compiler_params=params,
        cost_estimate=pl.CostEstimate(flops=10**8, bytes_accessed=10**6, transcendentals=0),
        name="unpack_own",
    )(own)
    shapes = [(3, WIDTH), (1, WIDTH), (3, WIDTH), (3, WIDTH), (3,), (3,)]
    hid_w, in_w, in_b, hid_b, out_w, out_b, means = pl.pallas_call(
        other_kernel,
        out_shape=[whole] + [jax.ShapeDtypeStruct(s, F32) for s in shapes],
        in_specs=[vmem, vmem, hbm],
        out_specs=[hbm] + [vmem] * 4 + [smem] * 2,
        scratch_shapes=scratch,
        input_output_aliases={2: 0},
        compiler_params=params,
        name="unpack_other",
    )(own, other, half_done)
    return in_w, in_b.reshape(WIDTH), hid_w, hid_b, out_w, out_b, means


def summed_over_devices(kept, given):
    mine = kept + lax.ppermute(given, NEAR, [(0, 1), (1, 0)])
    members = lax.axis_size(FAR)
    parts = lax.all_to_all(mine.reshape(members, HALF_ROWS // members, 128), FAR, 0, 0, tiled=True)
    own = parts.sum(axis=0)
    spread = jnp.broadcast_to(own[None], (members,) + own.shape)
    own = lax.all_to_all(spread, FAR, 0, 0, tiled=True).reshape(HALF_ROWS, 128)
    return own, lax.ppermute(own, NEAR, [(0, 1), (1, 0)])


def shards(
    point_data,
    point_counts,
    point_offsets,
    in_weight,
    input_bias,
    hidden_layer_weight,
    hidden_bias,
    output_weight,
    out_bias,
):
    kept, given = local_terms(
        point_counts,
        point_offsets,
        point_data,
        in_weight,
        input_bias,
        hidden_layer_weight,
        hidden_bias,
        output_weight,
        out_bias,
    )
    return unpacked(*summed_over_devices(kept, given))


def solution(mesh):
    torus = Mesh(mesh.devices.reshape(4, 4, 4, 2), PTS)
    placed = (P(None, PTS), P(PTS), P(PTS), P(), P(), P(), P(), P(), P())
    return jax.shard_map(
        shards,
        mesh=torus,
        in_specs=placed,
        out_specs=(P(), P(), P(), P(), P(), P(), P()),
        check_vma=False,
    )
```

```python
import functools

import jax
import jax.numpy as jnp
from jax import lax
from jax.experimental import pallas as pl
from jax.experimental.pallas import tpu as pltpu
from jax.sharding import Mesh
from jax.sharding import PartitionSpec as P

PTS = ("pts_0", "pts_1", "pts_2", "pts_3")
FAR = ("pts_0", "pts_1", "pts_2")
NEAR = "pts_3"

VISCOSITY = 0.2
HALF = 256
WIDTH = 256
ROWS = 16
F32 = jnp.float32
BF16 = jnp.bfloat16
JETS = 4
HALF_ROWS = 832
PIECES = (
    ((0, 0, 0, 256, 0), (0, 1, 0, 256, 256), (1, 0, 0, 256, 512), (1, 1, 0, 48, 768)),
    ((1, 1, 48, 208, 0), (2, 0, 0, 256, 208), (2, 1, 0, 256, 464)),
)
SMALL_ROW = 720
COUNT_ROWS = (816, 752)
TILES = [
    (slice(r * ROWS, (r + 1) * ROWS), slice(c * 128, (c + 1) * 128))
    for r in range(WIDTH // ROWS)
    for c in range(HALF // 128)
]
OFFSET = 3


def split(x):
    high = x.astype(BF16)
    return high, (x - high.astype(F32)).astype(BF16)


def matmul(a, b):
    return lax.dot_general(a, b, (((1,), (0,)), ((), ())), preferred_element_type=F32)


def matmul_nt(a, b):
    return lax.dot_general(a, b, (((1,), (1,)), ((), ())), preferred_element_type=F32)


def step_kernel(
    counts_ref,
    offsets_ref,
    data_hbm,
    in_w_hbm,
    in_b_hbm,
    hid_w_hbm,
    hid_b_hbm,
    out_w_hbm,
    out_b_hbm,
    kept_ref,
    given_ref,
    data_ref,
    in_w_ref,
    in_b_ref,
    hid_w_ref,
    hid_b_ref,
    out_w_ref,
    out_b_ref,
    copy_sems,
    w_cat,
    wt_cat,
    out_cat,
    outt_cat,
    cols,
    rows_buf,
    z_buf,
    h_buf,
    ah_buf,
    al_buf,
    a0h_buf,
    a0l_buf,
    g_buf,
    dzh_buf,
    dzl_buf,
    grads,
    partial,
    grad_out,
    sums_buf,
):
    copies = [
        pltpu.make_async_copy(source, target, copy_sems.at[i])
        for i, (source, target) in enumerate(
            (
                (in_w_hbm, in_w_ref),
                (in_b_hbm, in_b_ref),
                (hid_b_hbm, hid_b_ref),
                (out_w_hbm, out_w_ref),
                (hid_w_hbm, hid_w_ref),
                (data_hbm, data_ref),
                (out_b_hbm, out_b_ref),
            )
        )
    ]
    for copy in copies:
        copy.start()
    core = lax.axis_index(NEAR)
    grads[...] = jnp.zeros_like(grads)
    partial[...] = jnp.zeros_like(partial)
    sums_buf[...] = jnp.zeros_like(sums_buf)
    grad_out[...] = jnp.zeros_like(grad_out)
    out_cat[...] = jnp.zeros_like(out_cat)
    for copy in copies[:4]:
        copy.wait()

    wx = in_w_ref[0:1, :]
    wy = in_w_ref[1:2, :]
    rows = jnp.concatenate(
        [
            in_w_ref[...],
            in_b_ref[...],
            hid_b_ref[...],
            wx * wx + wy * wy,
        ],
        axis=0,
    )
    columns = rows.T
    for i in range(8):
        cols[i] = jnp.broadcast_to(columns[:, i : i + 1], (WIDTH, 128))

    for copy in copies[4:]:
        copy.wait()
    live_start = offsets_ref[0]
    live_count = counts_ref[0]
    first_block = live_start // (2 * HALF)
    end_block = (live_start + live_count + 2 * HALF - 1) // (2 * HALF)

    def put_cat(ref, index, value):
        high, low = split(value)
        ref[index, :, 0:256] = high
        ref[index, :, 256:512] = low
        ref[index, :, 512:768] = high

    w0 = hid_w_ref[0]
    for index, w in enumerate((w0, w0 * wx, w0 * wy, hid_w_ref[1], hid_w_ref[2])):
        put_cat(w_cat, index, w)
    for index, w in ((0, w0), (3, hid_w_ref[1]), (4, hid_w_ref[2])):
        turned = w.T
        put_cat(wt_cat, index, turned)
        if index == 0:
            for i in range(2):
                column = cols[i]
                put_cat(wt_cat, 1 + i, turned * jnp.concatenate([column, column], axis=1))
    out_high, out_low = split(out_w_ref[...])
    out_cat[0:3, 0:256] = out_high
    out_cat[0:3, 256:512] = out_high
    out_cat[16:19, 0:256] = out_low
    spare = jnp.zeros((5, WIDTH), F32)
    out_rows = jnp.concatenate(
        [out_high.astype(F32), spare, out_low.astype(F32), spare, out_high.astype(F32), spare, jnp.zeros((8, WIDTH), F32)],
        axis=0,
    )
    outt_cat[...] = out_rows.T.astype(BF16)
    def chain(base, at):
        points = data_ref[:, pl.ds(base, HALF)]
        slots = base + lax.broadcasted_iota(jnp.int32, (1, HALF), 1)
        mask = ((slots >= live_start) & (slots < live_start + live_count)).astype(F32)

        def spread(i, row):
            rows_buf[at, i] = jnp.broadcast_to(row, (8, HALF))

        def row(i, lane):
            tile = rows_buf[at, i, :, lane]
            return jnp.concatenate([tile, tile], axis=0)

        for i in range(3):
            spread(i, points[i : i + 1, :])

        def put_split(high_ref, low_ref, where, value):
            high, low = split(value)
            high_ref[where] = high
            low_ref[where] = low

        for r, l in TILES:
            z = cols[0, r] * row(0, l) + cols[1, r] * row(1, l) + cols[2, r] * row(2, l) + cols[3, r]
            h = jnp.tanh(z)
            s = 1.0 - h * h
            h_buf[at, 0, r, l] = h
            d = s * cols[2, r] + (2.0 * VISCOSITY) * (h * s) * cols[7, r]
            for i, a in enumerate((h, s, d)):
                put_split(a0h_buf, a0l_buf, (at, i, r, l), a)
        yield

        def source(layer, jet):
            if layer == 0:
                i = (0, 1, 1, 2)[jet]
                return a0h_buf[at, i], a0l_buf[at, i]
            return ah_buf[at, layer - 1, jet], al_buf[at, layer - 1, jet]

        for layer in range(3):
            for jet in range(JETS):
                high, low = source(layer, jet)
                w = w_cat[(0, 1, 2, 0)[jet]] if layer == 0 else w_cat[layer + 2]
                z_buf[at, layer, jet] = matmul(w, jnp.concatenate([high, high, low], axis=0))
            yield
            for r, l in TILES:
                h = jnp.tanh(z_buf[at, layer, 0, r, l] + cols[4 + layer, r])
                s = 1.0 - h * h
                h_buf[at, layer + 1, r, l] = h
                zx = z_buf[at, layer, 1, r, l]
                zy = z_buf[at, layer, 2, r, l]
                d = s * z_buf[at, layer, 3, r, l] + (2.0 * VISCOSITY) * (h * s) * (
                    zx * zx + zy * zy
                )
                for jet, a in enumerate((h, s * zx, s * zy, d)):
                    put_split(ah_buf, al_buf, (at, layer, jet, r, l), a)
            yield

        outs = []
        for jet in range(JETS):
            high, low = source(3, jet)
            both = matmul(out_cat[...], jnp.concatenate([high, low], axis=0))
            outs.append(both[0:8] + both[16:24])
        u = outs[0][0:1] + out_b_ref[0]
        v = outs[0][1:2] + out_b_ref[1]
        u_x, v_x, p_x = outs[1][0:1], outs[1][1:2], outs[1][2:3]
        u_y, v_y, p_y = outs[2][0:1], outs[2][1:2], outs[2][2:3]
        u_d, v_d = outs[3][0:1], outs[3][1:2]
        cont = mask * (u_x + v_y)
        mom_x = mask * (u_d + u * u_x + v * u_y + p_x - points[3:4, :])
        mom_y = mask * (v_d + u * v_x + v * v_y + p_y - points[4:5, :])
        gc = 4.0 * cont
        gx = 2.0 * mom_x
        gy = 2.0 * mom_y
        du = gx * u_x + gy * v_x
        dv = gx * u_y + gy * v_y
        nothing = jnp.zeros_like(gx)
        cotangents = [
            jnp.concatenate([a, b, c] + [nothing] * 5, axis=0)
            for a, b, c in (
                (du, dv, nothing),
                (gc + gx * u, gy * u, gx),
                (gx * v, gc + gy * v, gy),
                (gx, gy, nothing),
            )
        ]
        sums_buf[0:1, :] += cont * cont
        sums_buf[1:2, :] += mom_x * mom_x
        sums_buf[2:3, :] += mom_y * mom_y
        sums_buf[3:4, :] += du
        sums_buf[4:5, :] += dv
        left, right = [], []
        for jet, value in enumerate(cotangents):
            high = value.astype(BF16).astype(F32)
            low = value - high
            g_buf[at, jet] = matmul(
                outt_cat[...],
                jnp.concatenate([high, high, low, jnp.zeros_like(low)], axis=0).astype(BF16),
            )
            pad = jnp.zeros_like(high)
            both = jnp.concatenate([high, pad, low, pad], axis=0).astype(BF16)
            alone = jnp.concatenate([high, pad, pad, pad], axis=0).astype(BF16)
            a_high, a_low = source(3, jet)
            left += [both, alone]
            right += [a_high, a_low]
        grad_out[...] += matmul_nt(jnp.concatenate(left, axis=1), jnp.concatenate(right, axis=1))
        yield

        def activation_back(a, r, l):
            h = h_buf[at, a, r, l]
            s = 1.0 - h * h
            zx = z_buf[at, a - 1, 1, r, l]
            zy = z_buf[at, a - 1, 2, r, l]
            zd = z_buf[at, a - 1, 3, r, l]
            square = zx * zx + zy * zy
            g0, g1, g2, g3 = [g_buf[at, jet, r, l] for jet in range(JETS)]
            k = ((4.0 * VISCOSITY) * h) * g3
            d_s = zx * g1 + zy * g2 + zd * g3
            d_q = square * g3
            d0 = s * (g0 - 2.0 * (h * d_s) + (6.0 * VISCOSITY * s - 4.0 * VISCOSITY) * d_q)
            d1 = s * (g1 + k * zx)
            d2 = s * (g2 + k * zy)
            partial[a - 1, r] += d0
            for jet, d in enumerate((d0, d1, d2, s * g3)):
                put_split(dzh_buf, dzl_buf, (at, a % 2, jet, r, l), d)

        for r, l in TILES:
            activation_back(3, r, l)
        yield

        for layer in (2, 1):
            up = (layer + 1) % 2
            for jet in range(JETS):
                high = dzh_buf[at, up, jet]
                g_buf[at, jet] = matmul(
                    wt_cat[layer + 2],
                    jnp.concatenate([high, high, dzl_buf[at, up, jet]], axis=0),
                )
            left, right = [], []
            for jet in range(JETS):
                high = dzh_buf[at, up, jet]
                left += [high, dzl_buf[at, up, jet], high]
                a_high, a_low = source(layer, jet)
                right += [a_high, a_high, a_low]
            grads[layer + 2] += matmul_nt(
                jnp.concatenate(left, axis=1), jnp.concatenate(right, axis=1)
            )
            yield
            for r, l in TILES:
                activation_back(layer, r, l)
            yield

        def stacked(jet):
            high = dzh_buf[at, 1, jet]
            return [high, high, dzl_buf[at, 1, jet]]

        g_buf[at, 0] = matmul(wt_cat[0], jnp.concatenate(stacked(0), axis=0))
        g_buf[at, 1] = matmul(
            jnp.concatenate([wt_cat[1], wt_cat[2]], axis=1),
            jnp.concatenate(stacked(1) + stacked(2), axis=0),
        )
        g_buf[at, 2] = matmul(wt_cat[0], jnp.concatenate(stacked(3), axis=0))
        for index, jets in enumerate(((0, 3), (1,), (2,))):
            left, right = [], []
            for jet in jets:
                high = dzh_buf[at, 1, jet]
                left += [high, dzl_buf[at, 1, jet], high]
                a_high, a_low = source(0, jet)
                right += [a_high, a_high, a_low]
            grads[index] += matmul_nt(
                jnp.concatenate(left, axis=1), jnp.concatenate(right, axis=1)
            )
        yield
        for r, l in TILES:
            h = h_buf[at, 0, r, l]
            s = 1.0 - h * h
            g3 = g_buf[at, 2, r, l]
            d_s = g_buf[at, 1, r, l] + cols[2, r] * g3
            d_q = cols[7, r] * g3
            d = s * (
                g_buf[at, 0, r, l]
                - 2.0 * (h * d_s)
                + (6.0 * VISCOSITY * s - 4.0 * VISCOSITY) * d_q
            )
            partial[3, r] += d * row(0, l)
            partial[4, r] += d * row(1, l)
            partial[5, r] += d * row(2, l) + s * g3
            partial[6, r] += d
            partial[7, r] += (2.0 * VISCOSITY) * (h * s) * g3
        yield

    def run(chains):
        waiting = list(chains)
        at = 0
        while waiting:
            for k, stages in enumerate(chains):
                if stages in waiting and (k == 0 or at >= OFFSET):
                    if next(stages, "end") == "end":
                        waiting.remove(stages)
            at += 1

    def block(index, carry):
        base = pl.multiple_of(index * (2 * HALF), 2 * HALF)
        run([chain(pl.multiple_of(base + i * HALF, HALF), i) for i in range(2)])
        return carry

    lax.fori_loop(first_block, end_block, block, 0)

    wt = in_w_ref[2:3, :]
    grad0 = grads[0] + grads[1] * wx + grads[2] * wy
    direct = [
        jnp.sum(w0 * grads[1], axis=0, keepdims=True),
        jnp.sum(w0 * grads[2], axis=0, keepdims=True),
    ]
    lanes = lax.broadcasted_iota(jnp.int32, (WIDTH, 128), 1)
    placed = jnp.zeros((WIDTH, 128), F32)
    for i in range(8):
        placed = jnp.where(lanes == i, jnp.sum(partial[i], axis=1, keepdims=True), placed)
    small = placed.T[0:16]
    small_rows = [small[i : i + 1] for i in range(7)]
    small_rows.append(grad_out[0:3, :] + grad_out[16:19, :])
    by_square = 2.0 * small[7:8]
    small_rows[3] = small_rows[3] + direct[0] + by_square * wx
    small_rows[4] = small_rows[4] + direct[1] + by_square * wy
    totals = jnp.sum(sums_buf[...], axis=1, keepdims=True)
    lane = lax.broadcasted_iota(jnp.int32, (1, WIDTH), 1)
    scalars = jnp.zeros((1, WIDTH), F32)
    for at in range(5):
        scalars = jnp.where(lane == at, totals[at : at + 1], scalars)
    small_rows.append(scalars)
    block_small = jnp.concatenate(small_rows + [jnp.zeros((5, WIDTH), F32)], axis=0)
    count_rows = jnp.broadcast_to(live_count.astype(F32), (8, 128))

    def pack(refs):
        for ref, pieces, count_row in zip(refs, PIECES, COUNT_ROWS):
            for layer, side, first, rows, at in pieces:
                columns = slice(side * 128, side * 128 + 128)
                if layer == 0:
                    value = grad0[first : first + rows, columns]
                else:
                    value = grads[layer + 2, first : first + rows, columns]
                ref[at : at + rows, :] = value
            ref[count_row : count_row + 8, :] = count_rows
            ref[count_row + 8 :, :] = jnp.zeros((HALF_ROWS - count_row - 8, 128), F32)
        refs[1][SMALL_ROW : SMALL_ROW + 16, :] = block_small[:, :128]
        refs[1][SMALL_ROW + 16 : SMALL_ROW + 32, :] = block_small[:, 128:]

    @pl.when(core == 0)
    def _():
        pack((kept_ref, given_ref))

    @pl.when(core == 1)
    def _():
        pack((given_ref, kept_ref))


def local_terms(counts, offsets, data, in_w, in_b, hid_w, hid_b, out_w, out_b):
    vmem = pl.BlockSpec(memory_space=pltpu.VMEM)
    square = (WIDTH, HALF)
    half = jax.ShapeDtypeStruct((HALF_ROWS, 128), F32)
    inputs = [
        pltpu.with_memory_space_constraint(x, pltpu.HBM)
        for x in (data, in_w, in_b.reshape(1, WIDTH), hid_w, hid_b, out_w, out_b)
    ]
    return pl.pallas_call(
        step_kernel,
        out_shape=[half, half],
        in_specs=[pl.BlockSpec(memory_space=pltpu.SMEM)] * 2
        + [pl.BlockSpec(memory_space=pltpu.HBM)] * 7,
        out_specs=[vmem, vmem],
        scratch_shapes=[
            pltpu.VMEM(data.shape, F32),
            pltpu.VMEM((3, WIDTH), F32),
            pltpu.VMEM((1, WIDTH), F32),
            pltpu.VMEM((3, WIDTH, WIDTH), F32),
            pltpu.VMEM((3, WIDTH), F32),
            pltpu.VMEM((3, WIDTH), F32),
            pltpu.SMEM((3,), F32),
            pltpu.SemaphoreType.DMA((7,)),
            pltpu.VMEM((5, WIDTH, 768), BF16),
            pltpu.VMEM((5, WIDTH, 768), BF16),
            pltpu.VMEM((32, 512), BF16),
            pltpu.VMEM((WIDTH, 32), BF16),
            pltpu.VMEM((8, WIDTH, 128), F32),
            pltpu.VMEM((2, 3, 8, HALF), F32),
            pltpu.VMEM((2, 3, JETS) + square, F32),
            pltpu.VMEM((2, 4) + square, F32),
            pltpu.VMEM((2, 3, JETS) + square, BF16),
            pltpu.VMEM((2, 3, JETS) + square, BF16),
            pltpu.VMEM((2, 3) + square, BF16),
            pltpu.VMEM((2, 3) + square, BF16),
            pltpu.VMEM((2, JETS) + square, F32),
            pltpu.VMEM((2, 2, JETS) + square, BF16),
            pltpu.VMEM((2, 2, JETS) + square, BF16),
            pltpu.VMEM((5, WIDTH, WIDTH), F32),
            pltpu.VMEM((8, WIDTH, 128), F32),
            pltpu.VMEM((32, WIDTH), F32),
            pltpu.VMEM((8, HALF), F32),
        ],
        compiler_params=pltpu.CompilerParams(vmem_limit_bytes=44 * 1024 * 1024),
        name="pinn_step",
    )(counts, offsets, *inputs)


def put_half(ref, half, hid_w_hbm, buffer, copy_sems):
    scale = 1.0 / ref[COUNT_ROWS[half] : COUNT_ROWS[half] + 1, :]
    copies = []
    for i, (layer, side, first, rows, at) in enumerate(PIECES[half]):
        buffer[at : at + rows, :] = ref[at : at + rows, :] * scale
        copies.append(
            pltpu.make_async_copy(
                buffer.at[pl.ds(at, rows), :],
                hid_w_hbm.at[layer, pl.ds(first, rows), pl.ds(side * 128, 128)],
                copy_sems.at[i],
            )
        )
        copies[-1].start()
    return copies


def own_kernel(own_ref, hid_w_hbm, buffer, copy_sems):
    core = lax.axis_index(NEAR)
    for half in range(2):

        @pl.when(core == half)
        def _():
            for copy in put_half(own_ref, half, hid_w_hbm, buffer, copy_sems):
                copy.wait()


def other_kernel(
    own_ref, other_ref, _, hid_w_hbm, in_w, in_b, hid_b, out_w, out_b, means, buffer, copy_sems
):
    core = lax.axis_index(NEAR)

    def small(ref):
        scale = 1.0 / ref[COUNT_ROWS[1] : COUNT_ROWS[1] + 1, :]
        left = ref[SMALL_ROW : SMALL_ROW + 16, :] * scale
        right = ref[SMALL_ROW + 16 : SMALL_ROW + 32, :] * scale
        rows = jnp.concatenate([left, right], axis=1)
        hid_b[...] = rows[0:3]
        in_w[...] = rows[3:6]
        in_b[...] = rows[6:7]
        out_w[...] = rows[7:10]
        for i in range(3):
            means[i] = left[10, i]
            out_b[i] = left[10, 3 + i]

    for half in range(2):

        @pl.when(core == 1 - half)
        def _():
            copies = put_half(other_ref, half, hid_w_hbm, buffer, copy_sems)
            small((own_ref, other_ref)[half])
            for copy in copies:
                copy.wait()


def unpacked(own, other):
    vmem = pl.BlockSpec(memory_space=pltpu.VMEM)
    smem = pl.BlockSpec(memory_space=pltpu.SMEM)
    hbm = pl.BlockSpec(memory_space=pltpu.HBM)
    whole = jax.ShapeDtypeStruct((3, WIDTH, WIDTH), F32)
    scratch = [pltpu.VMEM((HALF_ROWS, 128), F32), pltpu.SemaphoreType.DMA((4,))]
    params = pltpu.CompilerParams(vmem_limit_bytes=8 * 1024 * 1024)
    half_done = pl.pallas_call(
        own_kernel,
        out_shape=whole,
        in_specs=[vmem],
        out_specs=hbm,
        scratch_shapes=scratch,
        compiler_params=params,
        cost_estimate=pl.CostEstimate(flops=10**8, bytes_accessed=10**6, transcendentals=0),
        name="unpack_own",
    )(own)
    shapes = [(3, WIDTH), (1, WIDTH), (3, WIDTH), (3, WIDTH), (3,), (3,)]
    hid_w, in_w, in_b, hid_b, out_w, out_b, means = pl.pallas_call(
        other_kernel,
        out_shape=[whole] + [jax.ShapeDtypeStruct(s, F32) for s in shapes],
        in_specs=[vmem, vmem, hbm],
        out_specs=[hbm] + [vmem] * 4 + [smem] * 2,
        scratch_shapes=scratch,
        input_output_aliases={2: 0},
        compiler_params=params,
        name="unpack_other",
    )(own, other, half_done)
    return in_w, in_b.reshape(WIDTH), hid_w, hid_b, out_w, out_b, means


def sum_kernel(members, parts_ref, spread_ref):
    rows = HALF_ROWS // members
    eight = 8 * rows
    groups = members // 8
    total = parts_ref[0:eight, :]
    for g in range(1, groups):
        total = total + parts_ref[g * eight : (g + 1) * eight, :]
    own = total[0:rows]
    for i in range(1, 8):
        own = own + total[i * rows : (i + 1) * rows]
    copies = jnp.concatenate([own] * 8, axis=0)
    for g in range(groups):
        spread_ref[g * eight : (g + 1) * eight, :] = copies


def sum_and_spread(parts, members):
    vmem = pl.BlockSpec(memory_space=pltpu.VMEM)
    return pl.pallas_call(
        functools.partial(sum_kernel, members),
        out_shape=jax.ShapeDtypeStruct(parts.shape, F32),
        in_specs=[vmem],
        out_specs=vmem,
        compiler_params=pltpu.CompilerParams(vmem_limit_bytes=4 * 1024 * 1024),
        name="sum_parts",
    )(parts)


def summed_over_devices(kept, given):
    mine = kept + lax.ppermute(given, NEAR, [(0, 1), (1, 0)])
    members = lax.axis_size(FAR)
    parts = lax.all_to_all(mine.reshape(HALF_ROWS, 1, 128), FAR, 0, 0, tiled=True)
    spread = sum_and_spread(parts.reshape(HALF_ROWS, 128), members)
    own = lax.all_to_all(spread.reshape(HALF_ROWS, 1, 128), FAR, 0, 0, tiled=True)
    own = own.reshape(HALF_ROWS, 128)
    return own, lax.ppermute(own, NEAR, [(0, 1), (1, 0)])


def shards(
    point_data,
    point_counts,
    point_offsets,
    in_weight,
    input_bias,
    hidden_layer_weight,
    hidden_bias,
    output_weight,
    out_bias,
):
    kept, given = local_terms(
        point_counts,
        point_offsets,
        point_data,
        in_weight,
        input_bias,
        hidden_layer_weight,
        hidden_bias,
        output_weight,
        out_bias,
    )
    return unpacked(*summed_over_devices(kept, given))


def solution(mesh):
    torus = Mesh(mesh.devices.reshape(4, 4, 4, 2), PTS)
    placed = (P(None, PTS), P(PTS), P(PTS), P(), P(), P(), P(), P(), P())
    return jax.shard_map(
        shards,
        mesh=torus,
        in_specs=placed,
        out_specs=(P(), P(), P(), P(), P(), P(), P()),
        check_vma=False,
    )
```

```python
import functools

import jax
import jax.numpy as jnp
from jax import lax
from jax.experimental import pallas as pl
from jax.experimental.pallas import tpu as pltpu
from jax.sharding import Mesh
from jax.sharding import PartitionSpec as P

PTS = ("pts_0", "pts_1", "pts_2", "pts_3")
FAR = ("pts_0", "pts_1", "pts_2")
NEAR = "pts_3"

VISCOSITY = 0.2
HALF = 256
WIDTH = 256
ROWS = 16
F32 = jnp.float32
BF16 = jnp.bfloat16
JETS = 4
HALF_ROWS = 832
PIECES = (
    ((0, 0, 0, 256, 0), (0, 1, 0, 256, 256), (1, 0, 0, 256, 512), (1, 1, 0, 48, 768)),
    ((1, 1, 48, 208, 0), (2, 0, 0, 256, 208), (2, 1, 0, 256, 464)),
)
SMALL_ROW = 720
COUNT_ROWS = (816, 752)
TILES = [
    (slice(r * ROWS, (r + 1) * ROWS), slice(c * 128, (c + 1) * 128))
    for r in range(WIDTH // ROWS)
    for c in range(HALF // 128)
]
OFFSET = 3


def split(x):
    high = x.astype(BF16)
    return high, (x - high.astype(F32)).astype(BF16)


def matmul(a, b):
    return lax.dot_general(a, b, (((1,), (0,)), ((), ())), preferred_element_type=F32)


def matmul_nt(a, b):
    return lax.dot_general(a, b, (((1,), (1,)), ((), ())), preferred_element_type=F32)


def step_kernel(
    counts_ref,
    offsets_ref,
    data_hbm,
    in_w_hbm,
    in_b_hbm,
    hid_w_hbm,
    hid_b_hbm,
    out_w_hbm,
    out_b_hbm,
    kept_ref,
    given_ref,
    data_ref,
    in_w_ref,
    in_b_ref,
    hid_w_ref,
    hid_b_ref,
    out_w_ref,
    out_b_ref,
    copy_sems,
    w_cat,
    wt_cat,
    out_cat,
    outt_cat,
    cols,
    rows_buf,
    z_buf,
    h_buf,
    ah_buf,
    al_buf,
    a0h_buf,
    a0l_buf,
    g_buf,
    dzh_buf,
    dzl_buf,
    grads,
    partial,
    grad_out,
    sums_buf,
):
    copies = [
        pltpu.make_async_copy(source, target, copy_sems.at[i])
        for i, (source, target) in enumerate(
            (
                (in_w_hbm, in_w_ref),
                (in_b_hbm, in_b_ref),
                (hid_b_hbm, hid_b_ref),
                (out_w_hbm, out_w_ref),
                (hid_w_hbm, hid_w_ref),
                (data_hbm, data_ref),
                (out_b_hbm, out_b_ref),
            )
        )
    ]
    for copy in copies:
        copy.start()
    core = lax.axis_index(NEAR)
    grads[...] = jnp.zeros_like(grads)
    partial[...] = jnp.zeros_like(partial)
    sums_buf[...] = jnp.zeros_like(sums_buf)
    grad_out[...] = jnp.zeros_like(grad_out)
    out_cat[...] = jnp.zeros_like(out_cat)
    for copy in copies[:4]:
        copy.wait()

    wx = in_w_ref[0:1, :]
    wy = in_w_ref[1:2, :]
    rows = jnp.concatenate(
        [
            in_w_ref[...],
            in_b_ref[...],
            hid_b_ref[...],
            wx * wx + wy * wy,
        ],
        axis=0,
    )
    columns = rows.T
    for i in range(8):
        cols[i] = jnp.broadcast_to(columns[:, i : i + 1], (WIDTH, 128))

    for copy in copies[4:]:
        copy.wait()
    live_start = offsets_ref[0]
    live_count = counts_ref[0]
    first_block = live_start // (2 * HALF)
    end_block = (live_start + live_count + 2 * HALF - 1) // (2 * HALF)

    def put_cat(ref, index, value):
        high, low = split(value)
        ref[index, :, 0:256] = high
        ref[index, :, 256:512] = low
        ref[index, :, 512:768] = high

    w0 = hid_w_ref[0]
    for index, w in enumerate((w0, w0 * wx, w0 * wy, hid_w_ref[1], hid_w_ref[2])):
        put_cat(w_cat, index, w)
    for index, w in ((0, w0), (3, hid_w_ref[1]), (4, hid_w_ref[2])):
        turned = w.T
        put_cat(wt_cat, index, turned)
        if index == 0:
            for i in range(2):
                column = cols[i]
                put_cat(wt_cat, 1 + i, turned * jnp.concatenate([column, column], axis=1))
    out_high, out_low = split(out_w_ref[...])
    out_cat[0:3, 0:256] = out_high
    out_cat[0:3, 256:512] = out_high
    out_cat[16:19, 0:256] = out_low
    spare = jnp.zeros((5, WIDTH), F32)
    out_rows = jnp.concatenate(
        [out_high.astype(F32), spare, out_low.astype(F32), spare, out_high.astype(F32), spare, jnp.zeros((8, WIDTH), F32)],
        axis=0,
    )
    outt_cat[...] = out_rows.T.astype(BF16)
    def chain(base, at):
        points = data_ref[:, pl.ds(base, HALF)]
        slots = base + lax.broadcasted_iota(jnp.int32, (1, HALF), 1)
        mask = ((slots >= live_start) & (slots < live_start + live_count)).astype(F32)

        def spread(i, row):
            rows_buf[at, i] = jnp.broadcast_to(row, (8, HALF))

        def row(i, lane):
            tile = rows_buf[at, i, :, lane]
            return jnp.concatenate([tile, tile], axis=0)

        for i in range(3):
            spread(i, points[i : i + 1, :])

        def put_split(high_ref, low_ref, where, value):
            high, low = split(value)
            high_ref[where] = high
            low_ref[where] = low

        for r, l in TILES:
            z = cols[0, r] * row(0, l) + cols[1, r] * row(1, l) + cols[2, r] * row(2, l) + cols[3, r]
            h = jnp.tanh(z)
            s = 1.0 - h * h
            h_buf[at, 0, r, l] = h
            d = s * cols[2, r] + (2.0 * VISCOSITY) * (h * s) * cols[7, r]
            for i, a in enumerate((h, s, d)):
                put_split(a0h_buf, a0l_buf, (at, i, r, l), a)
        yield

        def source(layer, jet):
            if layer == 0:
                i = (0, 1, 1, 2)[jet]
                return a0h_buf[at, i], a0l_buf[at, i]
            return ah_buf[at, layer - 1, jet], al_buf[at, layer - 1, jet]

        for layer in range(3):
            for jet in range(JETS):
                high, low = source(layer, jet)
                w = w_cat[(0, 1, 2, 0)[jet]] if layer == 0 else w_cat[layer + 2]
                z_buf[at, layer, jet] = matmul(w, jnp.concatenate([high, high, low], axis=0))
            yield
            for r, l in TILES:
                h = jnp.tanh(z_buf[at, layer, 0, r, l] + cols[4 + layer, r])
                s = 1.0 - h * h
                h_buf[at, layer + 1, r, l] = h
                zx = z_buf[at, layer, 1, r, l]
                zy = z_buf[at, layer, 2, r, l]
                d = s * z_buf[at, layer, 3, r, l] + (2.0 * VISCOSITY) * (h * s) * (
                    zx * zx + zy * zy
                )
                for jet, a in enumerate((h, s * zx, s * zy, d)):
                    put_split(ah_buf, al_buf, (at, layer, jet, r, l), a)
            yield

        outs = []
        for jet in range(JETS):
            high, low = source(3, jet)
            both = matmul(out_cat[...], jnp.concatenate([high, low], axis=0))
            outs.append(both[0:8] + both[16:24])
        u = outs[0][0:1] + out_b_ref[0]
        v = outs[0][1:2] + out_b_ref[1]
        u_x, v_x, p_x = outs[1][0:1], outs[1][1:2], outs[1][2:3]
        u_y, v_y, p_y = outs[2][0:1], outs[2][1:2], outs[2][2:3]
        u_d, v_d = outs[3][0:1], outs[3][1:2]
        cont = mask * (u_x + v_y)
        mom_x = mask * (u_d + u * u_x + v * u_y + p_x - points[3:4, :])
        mom_y = mask * (v_d + u * v_x + v * v_y + p_y - points[4:5, :])
        gc = 4.0 * cont
        gx = 2.0 * mom_x
        gy = 2.0 * mom_y
        du = gx * u_x + gy * v_x
        dv = gx * u_y + gy * v_y
        nothing = jnp.zeros_like(gx)
        cotangents = [
            jnp.concatenate([a, b, c] + [nothing] * 5, axis=0)
            for a, b, c in (
                (du, dv, nothing),
                (gc + gx * u, gy * u, gx),
                (gx * v, gc + gy * v, gy),
                (gx, gy, nothing),
            )
        ]
        sums_buf[0:1, :] += cont * cont
        sums_buf[1:2, :] += mom_x * mom_x
        sums_buf[2:3, :] += mom_y * mom_y
        sums_buf[3:4, :] += du
        sums_buf[4:5, :] += dv
        left, right = [], []
        for jet, value in enumerate(cotangents):
            high = value.astype(BF16).astype(F32)
            low = value - high
            g_buf[at, jet] = matmul(
                outt_cat[...],
                jnp.concatenate([high, high, low, jnp.zeros_like(low)], axis=0).astype(BF16),
            )
            pad = jnp.zeros_like(high)
            both = jnp.concatenate([high, pad, low, pad], axis=0).astype(BF16)
            alone = jnp.concatenate([high, pad, pad, pad], axis=0).astype(BF16)
            a_high, a_low = source(3, jet)
            left += [both, alone]
            right += [a_high, a_low]
        grad_out[...] += matmul_nt(jnp.concatenate(left, axis=1), jnp.concatenate(right, axis=1))
        yield

        def activation_back(a, r, l):
            h = h_buf[at, a, r, l]
            s = 1.0 - h * h
            zx = z_buf[at, a - 1, 1, r, l]
            zy = z_buf[at, a - 1, 2, r, l]
            zd = z_buf[at, a - 1, 3, r, l]
            square = zx * zx + zy * zy
            g0, g1, g2, g3 = [g_buf[at, jet, r, l] for jet in range(JETS)]
            k = ((4.0 * VISCOSITY) * h) * g3
            d_s = zx * g1 + zy * g2 + zd * g3
            d_q = square * g3
            d0 = s * (g0 - 2.0 * (h * d_s) + (6.0 * VISCOSITY * s - 4.0 * VISCOSITY) * d_q)
            d1 = s * (g1 + k * zx)
            d2 = s * (g2 + k * zy)
            partial[a - 1, r] += d0
            for jet, d in enumerate((d0, d1, d2, s * g3)):
                put_split(dzh_buf, dzl_buf, (at, a % 2, jet, r, l), d)

        for r, l in TILES:
            activation_back(3, r, l)
        yield

        for layer in (2, 1):
            up = (layer + 1) % 2
            for jet in range(JETS):
                high = dzh_buf[at, up, jet]
                g_buf[at, jet] = matmul(
                    wt_cat[layer + 2],
                    jnp.concatenate([high, high, dzl_buf[at, up, jet]], axis=0),
                )
            left, right = [], []
            for jet in range(JETS):
                high = dzh_buf[at, up, jet]
                left += [high, dzl_buf[at, up, jet], high]
                a_high, a_low = source(layer, jet)
                right += [a_high, a_high, a_low]
            grads[layer + 2] += matmul_nt(
                jnp.concatenate(left, axis=1), jnp.concatenate(right, axis=1)
            )
            yield
            for r, l in TILES:
                activation_back(layer, r, l)
            yield

        def stacked(jet):
            high = dzh_buf[at, 1, jet]
            return [high, high, dzl_buf[at, 1, jet]]

        g_buf[at, 0] = matmul(wt_cat[0], jnp.concatenate(stacked(0), axis=0))
        g_buf[at, 1] = matmul(
            jnp.concatenate([wt_cat[1], wt_cat[2]], axis=1),
            jnp.concatenate(stacked(1) + stacked(2), axis=0),
        )
        g_buf[at, 2] = matmul(wt_cat[0], jnp.concatenate(stacked(3), axis=0))
        for index, jets in enumerate(((0, 3), (1,), (2,))):
            left, right = [], []
            for jet in jets:
                high = dzh_buf[at, 1, jet]
                left += [high, dzl_buf[at, 1, jet], high]
                a_high, a_low = source(0, jet)
                right += [a_high, a_high, a_low]
            grads[index] += matmul_nt(
                jnp.concatenate(left, axis=1), jnp.concatenate(right, axis=1)
            )
        yield
        for r, l in TILES:
            h = h_buf[at, 0, r, l]
            s = 1.0 - h * h
            g3 = g_buf[at, 2, r, l]
            d_s = g_buf[at, 1, r, l] + cols[2, r] * g3
            d_q = cols[7, r] * g3
            d = s * (
                g_buf[at, 0, r, l]
                - 2.0 * (h * d_s)
                + (6.0 * VISCOSITY * s - 4.0 * VISCOSITY) * d_q
            )
            partial[3, r] += d * row(0, l)
            partial[4, r] += d * row(1, l)
            partial[5, r] += d * row(2, l) + s * g3
            partial[6, r] += d
            partial[7, r] += (2.0 * VISCOSITY) * (h * s) * g3
        yield

    def run(chains):
        waiting = list(chains)
        at = 0
        while waiting:
            for k, stages in enumerate(chains):
                if stages in waiting and (k == 0 or at >= OFFSET):
                    if next(stages, "end") == "end":
                        waiting.remove(stages)
            at += 1

    def block(index, carry):
        base = pl.multiple_of(index * (2 * HALF), 2 * HALF)
        run([chain(pl.multiple_of(base + i * HALF, HALF), i) for i in range(2)])
        return carry

    lax.fori_loop(first_block, end_block, block, 0)

    wt = in_w_ref[2:3, :]
    grad0 = grads[0] + grads[1] * wx + grads[2] * wy
    direct = [
        jnp.sum(w0 * grads[1], axis=0, keepdims=True),
        jnp.sum(w0 * grads[2], axis=0, keepdims=True),
    ]
    lanes = lax.broadcasted_iota(jnp.int32, (WIDTH, 128), 1)
    placed = jnp.zeros((WIDTH, 128), F32)
    for i in range(8):
        placed = jnp.where(lanes == i, jnp.sum(partial[i], axis=1, keepdims=True), placed)
    small = placed.T[0:16]
    small_rows = [small[i : i + 1] for i in range(7)]
    small_rows.append(grad_out[0:3, :] + grad_out[16:19, :])
    by_square = 2.0 * small[7:8]
    small_rows[3] = small_rows[3] + direct[0] + by_square * wx
    small_rows[4] = small_rows[4] + direct[1] + by_square * wy
    totals = jnp.sum(sums_buf[...], axis=1, keepdims=True)
    lane = lax.broadcasted_iota(jnp.int32, (1, WIDTH), 1)
    scalars = jnp.zeros((1, WIDTH), F32)
    for at in range(5):
        scalars = jnp.where(lane == at, totals[at : at + 1], scalars)
    small_rows.append(scalars)
    block_small = jnp.concatenate(small_rows + [jnp.zeros((5, WIDTH), F32)], axis=0)
    count_rows = jnp.broadcast_to(live_count.astype(F32), (8, 128))

    def pack(refs):
        for ref, pieces, count_row in zip(refs, PIECES, COUNT_ROWS):
            for layer, side, first, rows, at in pieces:
                columns = slice(side * 128, side * 128 + 128)
                if layer == 0:
                    value = grad0[first : first + rows, columns]
                else:
                    value = grads[layer + 2, first : first + rows, columns]
                ref[at : at + rows, :] = value
            ref[count_row : count_row + 8, :] = count_rows
            ref[count_row + 8 :, :] = jnp.zeros((HALF_ROWS - count_row - 8, 128), F32)
        refs[1][SMALL_ROW : SMALL_ROW + 16, :] = block_small[:, :128]
        refs[1][SMALL_ROW + 16 : SMALL_ROW + 32, :] = block_small[:, 128:]

    @pl.when(core == 0)
    def _():
        pack((kept_ref, given_ref))

    @pl.when(core == 1)
    def _():
        pack((given_ref, kept_ref))


def local_terms(counts, offsets, data, in_w, in_b, hid_w, hid_b, out_w, out_b):
    vmem = pl.BlockSpec(memory_space=pltpu.VMEM)
    square = (WIDTH, HALF)
    half = jax.ShapeDtypeStruct((HALF_ROWS, 128), F32)
    inputs = [
        pltpu.with_memory_space_constraint(x, pltpu.HBM)
        for x in (data, in_w, in_b.reshape(1, WIDTH), hid_w, hid_b, out_w, out_b)
    ]
    return pl.pallas_call(
        step_kernel,
        out_shape=[half, half],
        in_specs=[pl.BlockSpec(memory_space=pltpu.SMEM)] * 2
        + [pl.BlockSpec(memory_space=pltpu.HBM)] * 7,
        out_specs=[vmem, vmem],
        scratch_shapes=[
            pltpu.VMEM(data.shape, F32),
            pltpu.VMEM((3, WIDTH), F32),
            pltpu.VMEM((1, WIDTH), F32),
            pltpu.VMEM((3, WIDTH, WIDTH), F32),
            pltpu.VMEM((3, WIDTH), F32),
            pltpu.VMEM((3, WIDTH), F32),
            pltpu.SMEM((3,), F32),
            pltpu.SemaphoreType.DMA((7,)),
            pltpu.VMEM((5, WIDTH, 768), BF16),
            pltpu.VMEM((5, WIDTH, 768), BF16),
            pltpu.VMEM((32, 512), BF16),
            pltpu.VMEM((WIDTH, 32), BF16),
            pltpu.VMEM((8, WIDTH, 128), F32),
            pltpu.VMEM((2, 3, 8, HALF), F32),
            pltpu.VMEM((2, 3, JETS) + square, F32),
            pltpu.VMEM((2, 4) + square, F32),
            pltpu.VMEM((2, 3, JETS) + square, BF16),
            pltpu.VMEM((2, 3, JETS) + square, BF16),
            pltpu.VMEM((2, 3) + square, BF16),
            pltpu.VMEM((2, 3) + square, BF16),
            pltpu.VMEM((2, JETS) + square, F32),
            pltpu.VMEM((2, 2, JETS) + square, BF16),
            pltpu.VMEM((2, 2, JETS) + square, BF16),
            pltpu.VMEM((5, WIDTH, WIDTH), F32),
            pltpu.VMEM((8, WIDTH, 128), F32),
            pltpu.VMEM((32, WIDTH), F32),
            pltpu.VMEM((8, HALF), F32),
        ],
        compiler_params=pltpu.CompilerParams(vmem_limit_bytes=44 * 1024 * 1024),
        name="pinn_step",
    )(counts, offsets, *inputs)


def put_half(ref, half, hid_w_hbm, buffer, copy_sems):
    scale = 1.0 / ref[COUNT_ROWS[half] : COUNT_ROWS[half] + 1, :]
    copies = []
    for i, (layer, side, first, rows, at) in enumerate(PIECES[half]):
        buffer[at : at + rows, :] = ref[at : at + rows, :] * scale
        copies.append(
            pltpu.make_async_copy(
                buffer.at[pl.ds(at, rows), :],
                hid_w_hbm.at[layer, pl.ds(first, rows), pl.ds(side * 128, 128)],
                copy_sems.at[i],
            )
        )
        copies[-1].start()
    return copies


def own_kernel(own_ref, hid_w_hbm, buffer, copy_sems):
    core = lax.axis_index(NEAR)
    for half in range(2):

        @pl.when(core == half)
        def _():
            for copy in put_half(own_ref, half, hid_w_hbm, buffer, copy_sems):
                copy.wait()


def other_kernel(own_ref, other_ref, _, hid_w_hbm, *refs):
    small_hbm, small_refs = refs[:6], refs[6:12]
    buffer, copy_sems, small_sems = refs[12:]
    in_w, in_b, hid_b, out_w, out_b, means = small_refs
    core = lax.axis_index(NEAR)

    def small(ref):
        scale = 1.0 / ref[COUNT_ROWS[1] : COUNT_ROWS[1] + 1, :]
        left = ref[SMALL_ROW : SMALL_ROW + 16, :] * scale
        right = ref[SMALL_ROW + 16 : SMALL_ROW + 32, :] * scale
        rows = jnp.concatenate([left, right], axis=1)
        hid_b[...] = rows[0:3]
        in_w[...] = rows[3:6]
        in_b[...] = rows[6:7]
        out_w[...] = rows[7:10]
        for i in range(3):
            means[i] = left[10, i]
            out_b[i] = left[10, 3 + i]
        copies = [
            pltpu.make_async_copy(source, target, small_sems.at[i])
            for i, (source, target) in enumerate(zip(small_refs, small_hbm))
        ]
        for copy in copies:
            copy.start()
        return copies

    for half in range(2):

        @pl.when(core == 1 - half)
        def _():
            copies = put_half(other_ref, half, hid_w_hbm, buffer, copy_sems)
            copies += small((own_ref, other_ref)[half])
            for copy in copies:
                copy.wait()


def unpacked(own, other):
    vmem = pl.BlockSpec(memory_space=pltpu.VMEM)
    hbm = pl.BlockSpec(memory_space=pltpu.HBM)
    whole = jax.ShapeDtypeStruct((3, WIDTH, WIDTH), F32)
    scratch = [pltpu.VMEM((HALF_ROWS, 128), F32), pltpu.SemaphoreType.DMA((4,))]
    params = pltpu.CompilerParams(vmem_limit_bytes=8 * 1024 * 1024)
    half_done = pl.pallas_call(
        own_kernel,
        out_shape=whole,
        in_specs=[vmem],
        out_specs=hbm,
        scratch_shapes=scratch,
        compiler_params=params,
        cost_estimate=pl.CostEstimate(flops=10**8, bytes_accessed=10**6, transcendentals=0),
        name="unpack_own",
    )(own)
    shapes = [(3, WIDTH), (1, WIDTH), (3, WIDTH), (3, WIDTH), (3,), (3,)]
    hid_w, in_w, in_b, hid_b, out_w, out_b, means = pl.pallas_call(
        other_kernel,
        out_shape=[whole] + [jax.ShapeDtypeStruct(s, F32) for s in shapes],
        in_specs=[vmem, vmem, hbm],
        out_specs=[hbm] * 7,
        scratch_shapes=[pltpu.VMEM(s, F32) for s in shapes[:4]]
        + [pltpu.SMEM(s, F32) for s in shapes[4:]]
        + scratch
        + [pltpu.SemaphoreType.DMA((6,))],
        input_output_aliases={2: 0},
        compiler_params=params,
        name="unpack_other",
    )(own, other, half_done)
    return in_w, in_b.reshape(WIDTH), hid_w, hid_b, out_w, out_b, means


def sum_kernel(members, parts_ref, spread_ref):
    rows = HALF_ROWS // members
    eight = 8 * rows
    groups = members // 8
    total = parts_ref[0:eight, :]
    for g in range(1, groups):
        total = total + parts_ref[g * eight : (g + 1) * eight, :]
    own = total[0:rows]
    for i in range(1, 8):
        own = own + total[i * rows : (i + 1) * rows]
    copies = jnp.concatenate([own] * 8, axis=0)
    for g in range(groups):
        spread_ref[g * eight : (g + 1) * eight, :] = copies


def sum_and_spread(parts, members):
    vmem = pl.BlockSpec(memory_space=pltpu.VMEM)
    return pl.pallas_call(
        functools.partial(sum_kernel, members),
        out_shape=jax.ShapeDtypeStruct(parts.shape, F32),
        in_specs=[vmem],
        out_specs=vmem,
        compiler_params=pltpu.CompilerParams(vmem_limit_bytes=4 * 1024 * 1024),
        name="sum_parts",
    )(parts)


def summed_over_devices(kept, given):
    mine = kept + lax.ppermute(given, NEAR, [(0, 1), (1, 0)])
    members = lax.axis_size(FAR)
    parts = lax.all_to_all(mine.reshape(HALF_ROWS, 1, 128), FAR, 0, 0, tiled=True)
    spread = sum_and_spread(parts.reshape(HALF_ROWS, 128), members)
    own = lax.all_to_all(spread.reshape(HALF_ROWS, 1, 128), FAR, 0, 0, tiled=True)
    own = own.reshape(HALF_ROWS, 128)
    return own, lax.ppermute(own, NEAR, [(0, 1), (1, 0)])


def shards(
    point_data,
    point_counts,
    point_offsets,
    in_weight,
    input_bias,
    hidden_layer_weight,
    hidden_bias,
    output_weight,
    out_bias,
):
    kept, given = local_terms(
        point_counts,
        point_offsets,
        point_data,
        in_weight,
        input_bias,
        hidden_layer_weight,
        hidden_bias,
        output_weight,
        out_bias,
    )
    return unpacked(*summed_over_devices(kept, given))


def solution(mesh):
    torus = Mesh(mesh.devices.reshape(4, 4, 4, 2), PTS)
    placed = (P(None, PTS), P(PTS), P(PTS), P(), P(), P(), P(), P(), P())
    return jax.shard_map(
        shards,
        mesh=torus,
        in_specs=placed,
        out_specs=(P(), P(), P(), P(), P(), P(), P()),
        check_vma=False,
    )
```

```python
import functools

import jax
import jax.numpy as jnp
from jax import lax
from jax.experimental import pallas as pl
from jax.experimental.pallas import tpu as pltpu
from jax.sharding import Mesh
from jax.sharding import PartitionSpec as P

PTS = ("pts_0", "pts_1", "pts_2", "pts_3")
FAR = ("pts_0", "pts_1", "pts_2")
NEAR = "pts_3"

VISCOSITY = 0.2
HALF = 256
WIDTH = 256
ROWS = 32
F32 = jnp.float32
BF16 = jnp.bfloat16
JETS = 4
HALF_ROWS = 832
PIECES = (
    ((0, 0, 0, 256, 0), (0, 1, 0, 256, 256), (1, 0, 0, 256, 512), (1, 1, 0, 48, 768)),
    ((1, 1, 48, 208, 0), (2, 0, 0, 256, 208), (2, 1, 0, 256, 464)),
)
SMALL_ROW = 720
COUNT_ROWS = (816, 752)
TILES = [
    (slice(r * ROWS, (r + 1) * ROWS), slice(c * 128, (c + 1) * 128))
    for r in range(WIDTH // ROWS)
    for c in range(HALF // 128)
]
OFFSET = 3


def split(x):
    high = x.astype(BF16)
    return high, (x - high.astype(F32)).astype(BF16)


def matmul(a, b):
    return lax.dot_general(a, b, (((1,), (0,)), ((), ())), preferred_element_type=F32)


def matmul_nt(a, b):
    return lax.dot_general(a, b, (((1,), (1,)), ((), ())), preferred_element_type=F32)


def step_kernel(
    counts_ref,
    offsets_ref,
    data_hbm,
    in_w_hbm,
    in_b_hbm,
    hid_w_hbm,
    hid_b_hbm,
    out_w_hbm,
    out_b_hbm,
    kept_ref,
    given_ref,
    data_ref,
    in_w_ref,
    in_b_ref,
    hid_w_ref,
    hid_b_ref,
    out_w_ref,
    out_b_ref,
    copy_sems,
    w_cat,
    wt_cat,
    out_cat,
    outt_cat,
    cols,
    rows_buf,
    z_buf,
    h_buf,
    ah_buf,
    al_buf,
    a0h_buf,
    a0l_buf,
    g_buf,
    dzh_buf,
    dzl_buf,
    grads,
    partial,
    grad_out,
    sums_buf,
):
    copies = [
        pltpu.make_async_copy(source, target, copy_sems.at[i])
        for i, (source, target) in enumerate(
            (
                (in_w_hbm, in_w_ref),
                (in_b_hbm, in_b_ref),
                (hid_b_hbm, hid_b_ref),
                (out_w_hbm, out_w_ref),
                (hid_w_hbm, hid_w_ref),
                (data_hbm, data_ref),
                (out_b_hbm, out_b_ref),
            )
        )
    ]
    for copy in copies:
        copy.start()
    core = lax.axis_index(NEAR)
    grads[...] = jnp.zeros_like(grads)
    partial[...] = jnp.zeros_like(partial)
    sums_buf[...] = jnp.zeros_like(sums_buf)
    grad_out[...] = jnp.zeros_like(grad_out)
    out_cat[...] = jnp.zeros_like(out_cat)
    for copy in copies[:4]:
        copy.wait()

    wx = in_w_ref[0:1, :]
    wy = in_w_ref[1:2, :]
    rows = jnp.concatenate(
        [
            in_w_ref[...],
            in_b_ref[...],
            hid_b_ref[...],
            wx * wx + wy * wy,
        ],
        axis=0,
    )
    columns = rows.T
    for i in range(8):
        cols[i] = jnp.broadcast_to(columns[:, i : i + 1], (WIDTH, 128))

    for copy in copies[4:]:
        copy.wait()
    live_start = offsets_ref[0]
    live_count = counts_ref[0]
    first_block = live_start // (2 * HALF)
    end_block = (live_start + live_count + 2 * HALF - 1) // (2 * HALF)

    def put_cat(ref, index, value):
        high, low = split(value)
        ref[index, :, 0:256] = high
        ref[index, :, 256:512] = low
        ref[index, :, 512:768] = high

    w0 = hid_w_ref[0]
    for index, w in enumerate((w0, w0 * wx, w0 * wy, hid_w_ref[1], hid_w_ref[2])):
        put_cat(w_cat, index, w)
    for index, w in ((0, w0), (3, hid_w_ref[1]), (4, hid_w_ref[2])):
        turned = w.T
        put_cat(wt_cat, index, turned)
        if index == 0:
            for i in range(2):
                column = cols[i]
                put_cat(wt_cat, 1 + i, turned * jnp.concatenate([column, column], axis=1))
    out_high, out_low = split(out_w_ref[...])
    out_cat[0:3, 0:256] = out_high
    out_cat[0:3, 256:512] = out_high
    out_cat[16:19, 0:256] = out_low
    spare = jnp.zeros((5, WIDTH), F32)
    out_rows = jnp.concatenate(
        [out_high.astype(F32), spare, out_low.astype(F32), spare, out_high.astype(F32), spare, jnp.zeros((8, WIDTH), F32)],
        axis=0,
    )
    outt_cat[...] = out_rows.T.astype(BF16)
    def chain(base, at):
        points = data_ref[:, pl.ds(base, HALF)]
        slots = base + lax.broadcasted_iota(jnp.int32, (1, HALF), 1)
        mask = ((slots >= live_start) & (slots < live_start + live_count)).astype(F32)

        def spread(i, row):
            rows_buf[at, i] = jnp.broadcast_to(row, (8, HALF))

        def row(i, lane):
            tile = rows_buf[at, i, :, lane]
            return jnp.concatenate([tile] * (ROWS // 8), axis=0)

        for i in range(3):
            spread(i, points[i : i + 1, :])

        def put_split(high_ref, low_ref, where, value):
            high, low = split(value)
            high_ref[where] = high
            low_ref[where] = low

        for r, l in TILES:
            z = cols[0, r] * row(0, l) + cols[1, r] * row(1, l) + cols[2, r] * row(2, l) + cols[3, r]
            h = jnp.tanh(z)
            s = 1.0 - h * h
            h_buf[at, 0, r, l] = h
            d = s * cols[2, r] + (2.0 * VISCOSITY) * (h * s) * cols[7, r]
            for i, a in enumerate((h, s, d)):
                put_split(a0h_buf, a0l_buf, (at, i, r, l), a)
        yield

        def source(layer, jet):
            if layer == 0:
                i = (0, 1, 1, 2)[jet]
                return a0h_buf[at, i], a0l_buf[at, i]
            return ah_buf[at, layer - 1, jet], al_buf[at, layer - 1, jet]

        for layer in range(3):
            for jet in range(JETS):
                high, low = source(layer, jet)
                w = w_cat[(0, 1, 2, 0)[jet]] if layer == 0 else w_cat[layer + 2]
                z_buf[at, layer, jet] = matmul(w, jnp.concatenate([high, high, low], axis=0))
            yield
            for r, l in TILES:
                h = jnp.tanh(z_buf[at, layer, 0, r, l] + cols[4 + layer, r])
                s = 1.0 - h * h
                h_buf[at, layer + 1, r, l] = h
                zx = z_buf[at, layer, 1, r, l]
                zy = z_buf[at, layer, 2, r, l]
                d = s * z_buf[at, layer, 3, r, l] + (2.0 * VISCOSITY) * (h * s) * (
                    zx * zx + zy * zy
                )
                for jet, a in enumerate((h, s * zx, s * zy, d)):
                    put_split(ah_buf, al_buf, (at, layer, jet, r, l), a)
            yield

        outs = []
        for jet in range(JETS):
            high, low = source(3, jet)
            both = matmul(out_cat[...], jnp.concatenate([high, low], axis=0))
            outs.append(both[0:8] + both[16:24])
        u = outs[0][0:1] + out_b_ref[0]
        v = outs[0][1:2] + out_b_ref[1]
        u_x, v_x, p_x = outs[1][0:1], outs[1][1:2], outs[1][2:3]
        u_y, v_y, p_y = outs[2][0:1], outs[2][1:2], outs[2][2:3]
        u_d, v_d = outs[3][0:1], outs[3][1:2]
        cont = mask * (u_x + v_y)
        mom_x = mask * (u_d + u * u_x + v * u_y + p_x - points[3:4, :])
        mom_y = mask * (v_d + u * v_x + v * v_y + p_y - points[4:5, :])
        gc = 4.0 * cont
        gx = 2.0 * mom_x
        gy = 2.0 * mom_y
        du = gx * u_x + gy * v_x
        dv = gx * u_y + gy * v_y
        nothing = jnp.zeros_like(gx)
        cotangents = [
            jnp.concatenate([a, b, c] + [nothing] * 5, axis=0)
            for a, b, c in (
                (du, dv, nothing),
                (gc + gx * u, gy * u, gx),
                (gx * v, gc + gy * v, gy),
                (gx, gy, nothing),
            )
        ]
        sums_buf[0:1, :] += cont * cont
        sums_buf[1:2, :] += mom_x * mom_x
        sums_buf[2:3, :] += mom_y * mom_y
        sums_buf[3:4, :] += du
        sums_buf[4:5, :] += dv
        left, right = [], []
        for jet, value in enumerate(cotangents):
            high = value.astype(BF16).astype(F32)
            low = value - high
            g_buf[at, jet] = matmul(
                outt_cat[...],
                jnp.concatenate([high, high, low, jnp.zeros_like(low)], axis=0).astype(BF16),
            )
            pad = jnp.zeros_like(high)
            both = jnp.concatenate([high, pad, low, pad], axis=0).astype(BF16)
            alone = jnp.concatenate([high, pad, pad, pad], axis=0).astype(BF16)
            a_high, a_low = source(3, jet)
            left += [both, alone]
            right += [a_high, a_low]
        grad_out[...] += matmul_nt(jnp.concatenate(left, axis=1), jnp.concatenate(right, axis=1))
        yield

        def activation_back(a, r, l):
            h = h_buf[at, a, r, l]
            s = 1.0 - h * h
            zx = z_buf[at, a - 1, 1, r, l]
            zy = z_buf[at, a - 1, 2, r, l]
            zd = z_buf[at, a - 1, 3, r, l]
            square = zx * zx + zy * zy
            g0, g1, g2, g3 = [g_buf[at, jet, r, l] for jet in range(JETS)]
            k = ((4.0 * VISCOSITY) * h) * g3
            d_s = zx * g1 + zy * g2 + zd * g3
            d_q = square * g3
            d0 = s * (g0 - 2.0 * (h * d_s) + (6.0 * VISCOSITY * s - 4.0 * VISCOSITY) * d_q)
            d1 = s * (g1 + k * zx)
            d2 = s * (g2 + k * zy)
            partial[a - 1, r] += d0
            for jet, d in enumerate((d0, d1, d2, s * g3)):
                put_split(dzh_buf, dzl_buf, (at, a % 2, jet, r, l), d)

        for r, l in TILES:
            activation_back(3, r, l)
        yield

        for layer in (2, 1):
            up = (layer + 1) % 2
            for jet in range(JETS):
                high = dzh_buf[at, up, jet]
                g_buf[at, jet] = matmul(
                    wt_cat[layer + 2],
                    jnp.concatenate([high, high, dzl_buf[at, up, jet]], axis=0),
                )
            left, right = [], []
            for jet in range(JETS):
                high = dzh_buf[at, up, jet]
                left += [high, dzl_buf[at, up, jet], high]
                a_high, a_low = source(layer, jet)
                right += [a_high, a_high, a_low]
            grads[layer + 2] += matmul_nt(
                jnp.concatenate(left, axis=1), jnp.concatenate(right, axis=1)
            )
            yield
            for r, l in TILES:
                activation_back(layer, r, l)
            yield

        def stacked(jet):
            high = dzh_buf[at, 1, jet]
            return [high, high, dzl_buf[at, 1, jet]]

        g_buf[at, 0] = matmul(wt_cat[0], jnp.concatenate(stacked(0), axis=0))
        g_buf[at, 1] = matmul(
            jnp.concatenate([wt_cat[1], wt_cat[2]], axis=1),
            jnp.concatenate(stacked(1) + stacked(2), axis=0),
        )
        g_buf[at, 2] = matmul(wt_cat[0], jnp.concatenate(stacked(3), axis=0))
        for index, jets in enumerate(((0, 3), (1,), (2,))):
            left, right = [], []
            for jet in jets:
                high = dzh_buf[at, 1, jet]
                left += [high, dzl_buf[at, 1, jet], high]
                a_high, a_low = source(0, jet)
                right += [a_high, a_high, a_low]
            grads[index] += matmul_nt(
                jnp.concatenate(left, axis=1), jnp.concatenate(right, axis=1)
            )
        yield
        for r, l in TILES:
            h = h_buf[at, 0, r, l]
            s = 1.0 - h * h
            g3 = g_buf[at, 2, r, l]
            d_s = g_buf[at, 1, r, l] + cols[2, r] * g3
            d_q = cols[7, r] * g3
            d = s * (
                g_buf[at, 0, r, l]
                - 2.0 * (h * d_s)
                + (6.0 * VISCOSITY * s - 4.0 * VISCOSITY) * d_q
            )
            partial[3, r] += d * row(0, l)
            partial[4, r] += d * row(1, l)
            partial[5, r] += d * row(2, l) + s * g3
            partial[6, r] += d
            partial[7, r] += (2.0 * VISCOSITY) * (h * s) * g3
        yield

    def run(chains):
        waiting = list(chains)
        at = 0
        while waiting:
            for k, stages in enumerate(chains):
                if stages in waiting and (k == 0 or at >= OFFSET):
                    if next(stages, "end") == "end":
                        waiting.remove(stages)
            at += 1

    def block(index, carry):
        base = pl.multiple_of(index * (2 * HALF), 2 * HALF)
        run([chain(pl.multiple_of(base + i * HALF, HALF), i) for i in range(2)])
        return carry

    lax.fori_loop(first_block, end_block, block, 0)

    wt = in_w_ref[2:3, :]
    grad0 = grads[0] + grads[1] * wx + grads[2] * wy
    direct = [
        jnp.sum(w0 * grads[1], axis=0, keepdims=True),
        jnp.sum(w0 * grads[2], axis=0, keepdims=True),
    ]
    lanes = lax.broadcasted_iota(jnp.int32, (WIDTH, 128), 1)
    placed = jnp.zeros((WIDTH, 128), F32)
    for i in range(8):
        placed = jnp.where(lanes == i, jnp.sum(partial[i], axis=1, keepdims=True), placed)
    small = placed.T[0:16]
    small_rows = [small[i : i + 1] for i in range(7)]
    small_rows.append(grad_out[0:3, :] + grad_out[16:19, :])
    by_square = 2.0 * small[7:8]
    small_rows[3] = small_rows[3] + direct[0] + by_square * wx
    small_rows[4] = small_rows[4] + direct[1] + by_square * wy
    totals = jnp.sum(sums_buf[...], axis=1, keepdims=True)
    lane = lax.broadcasted_iota(jnp.int32, (1, WIDTH), 1)
    scalars = jnp.zeros((1, WIDTH), F32)
    for at in range(5):
        scalars = jnp.where(lane == at, totals[at : at + 1], scalars)
    small_rows.append(scalars)
    block_small = jnp.concatenate(small_rows + [jnp.zeros((5, WIDTH), F32)], axis=0)
    count_rows = jnp.broadcast_to(live_count.astype(F32), (8, 128))

    def pack(refs):
        for ref, pieces, count_row in zip(refs, PIECES, COUNT_ROWS):
            for layer, side, first, rows, at in pieces:
                columns = slice(side * 128, side * 128 + 128)
                if layer == 0:
                    value = grad0[first : first + rows, columns]
                else:
                    value = grads[layer + 2, first : first + rows, columns]
                ref[at : at + rows, :] = value
            ref[count_row : count_row + 8, :] = count_rows
            ref[count_row + 8 :, :] = jnp.zeros((HALF_ROWS - count_row - 8, 128), F32)
        refs[1][SMALL_ROW : SMALL_ROW + 16, :] = block_small[:, :128]
        refs[1][SMALL_ROW + 16 : SMALL_ROW + 32, :] = block_small[:, 128:]

    @pl.when(core == 0)
    def _():
        pack((kept_ref, given_ref))

    @pl.when(core == 1)
    def _():
        pack((given_ref, kept_ref))


def local_terms(counts, offsets, data, in_w, in_b, hid_w, hid_b, out_w, out_b):
    vmem = pl.BlockSpec(memory_space=pltpu.VMEM)
    square = (WIDTH, HALF)
    half = jax.ShapeDtypeStruct((HALF_ROWS, 128), F32)
    inputs = [
        pltpu.with_memory_space_constraint(x, pltpu.HBM)
        for x in (data, in_w, in_b.reshape(1, WIDTH), hid_w, hid_b, out_w, out_b)
    ]
    return pl.pallas_call(
        step_kernel,
        out_shape=[half, half],
        in_specs=[pl.BlockSpec(memory_space=pltpu.SMEM)] * 2
        + [pl.BlockSpec(memory_space=pltpu.HBM)] * 7,
        out_specs=[vmem, vmem],
        scratch_shapes=[
            pltpu.VMEM(data.shape, F32),
            pltpu.VMEM((3, WIDTH), F32),
            pltpu.VMEM((1, WIDTH), F32),
            pltpu.VMEM((3, WIDTH, WIDTH), F32),
            pltpu.VMEM((3, WIDTH), F32),
            pltpu.VMEM((3, WIDTH), F32),
            pltpu.SMEM((3,), F32),
            pltpu.SemaphoreType.DMA((7,)),
            pltpu.VMEM((5, WIDTH, 768), BF16),
            pltpu.VMEM((5, WIDTH, 768), BF16),
            pltpu.VMEM((32, 512), BF16),
            pltpu.VMEM((WIDTH, 32), BF16),
            pltpu.VMEM((8, WIDTH, 128), F32),
            pltpu.VMEM((2, 3, 8, HALF), F32),
            pltpu.VMEM((2, 3, JETS) + square, F32),
            pltpu.VMEM((2, 4) + square, F32),
            pltpu.VMEM((2, 3, JETS) + square, BF16),
            pltpu.VMEM((2, 3, JETS) + square, BF16),
            pltpu.VMEM((2, 3) + square, BF16),
            pltpu.VMEM((2, 3) + square, BF16),
            pltpu.VMEM((2, JETS) + square, F32),
            pltpu.VMEM((2, 2, JETS) + square, BF16),
            pltpu.VMEM((2, 2, JETS) + square, BF16),
            pltpu.VMEM((5, WIDTH, WIDTH), F32),
            pltpu.VMEM((8, WIDTH, 128), F32),
            pltpu.VMEM((32, WIDTH), F32),
            pltpu.VMEM((8, HALF), F32),
        ],
        compiler_params=pltpu.CompilerParams(vmem_limit_bytes=44 * 1024 * 1024),
        name="pinn_step",
    )(counts, offsets, *inputs)


def put_half(ref, half, hid_w_hbm, buffer, copy_sems):
    scale = 1.0 / ref[COUNT_ROWS[half] : COUNT_ROWS[half] + 1, :]
    copies = []
    for i, (layer, side, first, rows, at) in enumerate(PIECES[half]):
        buffer[at : at + rows, :] = ref[at : at + rows, :] * scale
        copies.append(
            pltpu.make_async_copy(
                buffer.at[pl.ds(at, rows), :],
                hid_w_hbm.at[layer, pl.ds(first, rows), pl.ds(side * 128, 128)],
                copy_sems.at[i],
            )
        )
        copies[-1].start()
    return copies


def own_kernel(own_ref, hid_w_hbm, buffer, copy_sems):
    core = lax.axis_index(NEAR)
    for half in range(2):

        @pl.when(core == half)
        def _():
            for copy in put_half(own_ref, half, hid_w_hbm, buffer, copy_sems):
                copy.wait()


def other_kernel(own_ref, other_ref, _, hid_w_hbm, *refs):
    small_hbm, small_refs = refs[:6], refs[6:12]
    buffer, copy_sems, small_sems = refs[12:]
    in_w, in_b, hid_b, out_w, out_b, means = small_refs
    core = lax.axis_index(NEAR)

    def small(ref):
        scale = 1.0 / ref[COUNT_ROWS[1] : COUNT_ROWS[1] + 1, :]
        left = ref[SMALL_ROW : SMALL_ROW + 16, :] * scale
        right = ref[SMALL_ROW + 16 : SMALL_ROW + 32, :] * scale
        rows = jnp.concatenate([left, right], axis=1)
        hid_b[...] = rows[0:3]
        in_w[...] = rows[3:6]
        in_b[...] = rows[6:7]
        out_w[...] = rows[7:10]
        for i in range(3):
            means[i] = left[10, i]
            out_b[i] = left[10, 3 + i]
        copies = [
            pltpu.make_async_copy(source, target, small_sems.at[i])
            for i, (source, target) in enumerate(zip(small_refs, small_hbm))
        ]
        for copy in copies:
            copy.start()
        return copies

    for half in range(2):

        @pl.when(core == 1 - half)
        def _():
            copies = put_half(other_ref, half, hid_w_hbm, buffer, copy_sems)
            copies += small((own_ref, other_ref)[half])
            for copy in copies:
                copy.wait()


def unpacked(own, other):
    vmem = pl.BlockSpec(memory_space=pltpu.VMEM)
    hbm = pl.BlockSpec(memory_space=pltpu.HBM)
    whole = jax.ShapeDtypeStruct((3, WIDTH, WIDTH), F32)
    scratch = [pltpu.VMEM((HALF_ROWS, 128), F32), pltpu.SemaphoreType.DMA((4,))]
    params = pltpu.CompilerParams(vmem_limit_bytes=8 * 1024 * 1024)
    half_done = pl.pallas_call(
        own_kernel,
        out_shape=whole,
        in_specs=[vmem],
        out_specs=hbm,
        scratch_shapes=scratch,
        compiler_params=params,
        cost_estimate=pl.CostEstimate(flops=10**8, bytes_accessed=10**6, transcendentals=0),
        name="unpack_own",
    )(own)
    shapes = [(3, WIDTH), (1, WIDTH), (3, WIDTH), (3, WIDTH), (3,), (3,)]
    hid_w, in_w, in_b, hid_b, out_w, out_b, means = pl.pallas_call(
        other_kernel,
        out_shape=[whole] + [jax.ShapeDtypeStruct(s, F32) for s in shapes],
        in_specs=[vmem, vmem, hbm],
        out_specs=[hbm] * 7,
        scratch_shapes=[pltpu.VMEM(s, F32) for s in shapes[:4]]
        + [pltpu.SMEM(s, F32) for s in shapes[4:]]
        + scratch
        + [pltpu.SemaphoreType.DMA((6,))],
        input_output_aliases={2: 0},
        compiler_params=params,
        name="unpack_other",
    )(own, other, half_done)
    return in_w, in_b.reshape(WIDTH), hid_w, hid_b, out_w, out_b, means


def sum_kernel(members, parts_ref, spread_ref):
    rows = HALF_ROWS // members
    eight = 8 * rows
    groups = members // 8
    total = parts_ref[0:eight, :]
    for g in range(1, groups):
        total = total + parts_ref[g * eight : (g + 1) * eight, :]
    own = total[0:rows]
    for i in range(1, 8):
        own = own + total[i * rows : (i + 1) * rows]
    copies = jnp.concatenate([own] * 8, axis=0)
    for g in range(groups):
        spread_ref[g * eight : (g + 1) * eight, :] = copies


def sum_and_spread(parts, members):
    vmem = pl.BlockSpec(memory_space=pltpu.VMEM)
    return pl.pallas_call(
        functools.partial(sum_kernel, members),
        out_shape=jax.ShapeDtypeStruct(parts.shape, F32),
        in_specs=[vmem],
        out_specs=vmem,
        compiler_params=pltpu.CompilerParams(vmem_limit_bytes=4 * 1024 * 1024),
        name="sum_parts",
    )(parts)


def summed_over_devices(kept, given):
    mine = kept + lax.ppermute(given, NEAR, [(0, 1), (1, 0)])
    members = lax.axis_size(FAR)
    parts = lax.all_to_all(mine.reshape(HALF_ROWS, 1, 128), FAR, 0, 0, tiled=True)
    spread = sum_and_spread(parts.reshape(HALF_ROWS, 128), members)
    own = lax.all_to_all(spread.reshape(HALF_ROWS, 1, 128), FAR, 0, 0, tiled=True)
    own = own.reshape(HALF_ROWS, 128)
    return own, lax.ppermute(own, NEAR, [(0, 1), (1, 0)])


def shards(
    point_data,
    point_counts,
    point_offsets,
    in_weight,
    input_bias,
    hidden_layer_weight,
    hidden_bias,
    output_weight,
    out_bias,
):
    kept, given = local_terms(
        point_counts,
        point_offsets,
        point_data,
        in_weight,
        input_bias,
        hidden_layer_weight,
        hidden_bias,
        output_weight,
        out_bias,
    )
    return unpacked(*summed_over_devices(kept, given))


def solution(mesh):
    torus = Mesh(mesh.devices.reshape(4, 4, 4, 2), PTS)
    placed = (P(None, PTS), P(PTS), P(PTS), P(), P(), P(), P(), P(), P())
    return jax.shard_map(
        shards,
        mesh=torus,
        in_specs=placed,
        out_specs=(P(), P(), P(), P(), P(), P(), P()),
        check_vma=False,
    )
```
